128 devices in a mesh: gx: 8 (over y_hi, z), gy: 4 (over x), gz: 4 (over y_lo, core).
Axes of the slice: x: 4, y: 4 (y_hi: 2, y_lo: 2; y = y_hi * 2 + y_lo), z: 4, core: 2. Of those that a mesh axis runs over, the one named last changes fastest.
Arguments:
- density: float32 [128, 64, 512], P('gx', 'gy', 'gz'), may hold values from 0.005 to 0.6, as said below
- coupling: float32 [14, 14], replicated, may hold values from -0.3 to 1.5, as said below
Outputs:
- potentials: float32 [14, 128, 64, 512], P(None, 'gx', 'gy', 'gz')
The draws below stay inside these ranges and needn't reach their ends.
Inputs may be any that keep to these rules, and one draw needn't show every extreme that they name: Positive density. `coupling`: symmetric.
All inputs are finite; a program needn't handle non-finite values.
Results may differ from the reference program's by a relative error of at most 0.0003.
Values sent between devices are 32-bit elements; how exact they have to be, the bound alone decides.
A program may use at most 128 MiB of HBM per device.

```python
import math
import jax
import jax.numpy as jnp
from jax import lax

NQ = 14
NX = 128
NY = 64
NZ = 512


def draw_density(key, part):
    rough_key = jax.random.fold_in(key, 11)
    along_x = jnp.arange(NX, dtype=jnp.float32) / NX
    along_y = jnp.arange(NY, dtype=jnp.float32) / NY
    along_z = jnp.arange(NZ, dtype=jnp.float32) / NZ
    envelope = (along_x[:, None, None] + 0.7 * along_y[None, :, None] + 0.5 * along_z[None, None, :]) / 2.2
    roughness = jax.random.uniform(rough_key, (NX, NY, NZ), jnp.float32, -1.0, 1.0)
    return 0.01 * jnp.exp(math.log(40.0) * envelope) * (1.0 + 0.5 * roughness)


def draw_coupling(key, part):
    base_key = jax.random.fold_in(key, 23)
    diag_key = jax.random.fold_in(key, 29)
    entries = jax.random.uniform(base_key, (NQ, NQ), jnp.float32, -1.0, 1.0)
    diagonal = jax.random.uniform(diag_key, (NQ,), jnp.float32, 0.8, 1.2)
    return 0.15 * (entries + entries.T) + jnp.diag(diagonal)


def setup_inputs(seed: int = 0) -> dict:
    key_of = jax.random.split(jax.random.key(seed), 3)
    density = draw_density(jax.random.fold_in(key_of[2], 71), 0)
    coupling = draw_coupling(jax.random.fold_in(key_of[2], 71), 0)
    return dict(density=density, coupling=coupling)


zab_ratio = 0.8491 / 9.0
q_cut = 5.0
mesh_step = 0.07
range_factor = 1.0
local_weight = 0.25
spline_root = math.sqrt(3.0) - 2.0
highest = lax.Precision.HIGHEST

def gradient_squared(density):
    summed = jnp.zeros_like(density)
    for dim_index in range(3):
        nearer = jnp.roll(density, -1, dim_index) - jnp.roll(density, 1, dim_index)
        farther = jnp.roll(density, -2, dim_index) - jnp.roll(density, 2, dim_index)
        gradient = (8.0 * nearer - farther) / 12.0
        summed = summed + gradient * gradient
    return summed

def saturated_wavevector(density, grad_sq):
    fermi_k = jnp.cbrt(3.0 * math.pi * math.pi * density)
    reduced = grad_sq / (4.0 * fermi_k * fermi_k * density * density)
    raw_q = fermi_k * (1.0 + zab_ratio * reduced)
    scaled = raw_q / q_cut
    powered = scaled
    series = jnp.zeros_like(scaled)
    for term_order in range(1, 13):
        series = series + powered / term_order
        powered = powered * scaled
    return q_cut * (1.0 - jnp.exp(-series))

def spline_weights(q_zero, q_top, qpoints):
    position = jnp.maximum(qpoints - 1.0 + jnp.log(q_zero / q_top) / mesh_step, 0.0)
    knot_ids = jnp.arange(-1, qpoints + 1, dtype=jnp.int32)
    offset = jnp.abs(position[None, :] - knot_ids.astype(jnp.float32)[:, None])
    bspline = (jnp.maximum(2.0 - offset, 0.0) ** 3 - 4.0 * jnp.maximum(1.0 - offset, 0.0) ** 3) / 6.0
    q_nodes = jnp.arange(qpoints, dtype=jnp.int32)
    distance = jnp.abs(knot_ids[:, None] - q_nodes[None, :])
    parity = (1 - 2 * (distance % 2)).astype(jnp.float32)
    matrix = math.sqrt(3.0) * parity * jnp.exp(distance.astype(jnp.float32) * math.log(-spline_root))
    return jnp.dot(matrix.T, bspline, precision=highest)

def wave_squared(wave_ids, length):
    folded = jnp.where(2 * wave_ids < length, wave_ids, wave_ids - length)
    wavenum = 2.0 * math.pi / length * folded.astype(jnp.float32)
    return wavenum * wavenum

def reference(density, coupling):
    qpoints = coupling.shape[0]
    grad_sq = gradient_squared(density)
    q_zero = saturated_wavevector(density, grad_sq)
    q_top = jnp.max(q_zero)

    def one_plane(x_plane):
        dens_plane, q_plane = x_plane
        weights = spline_weights(q_plane.reshape(-1), q_top, qpoints)
        return weights * dens_plane.reshape(1, -1)
    thetas = lax.map(one_plane, (density, q_zero))
    thetas = jnp.transpose(thetas, (1, 0, 2)).reshape(qpoints, NX, NY, NZ)
    spectra = jnp.fft.fftn(thetas, axes=(1, 2, 3))
    k_squared = wave_squared(jnp.arange(NX, dtype=jnp.int32), NX)[:, None, None] + wave_squared(jnp.arange(NY, dtype=jnp.int32), NY)[None, :, None] + wave_squared(jnp.arange(NZ, dtype=jnp.int32), NZ)[None, None, :]
    q_nodes = jnp.arange(qpoints, dtype=jnp.int32)
    q_mesh = q_top * jnp.exp(-mesh_step * (qpoints - 1 - q_nodes).astype(jnp.float32))
    masses = range_factor * q_mesh[:, None] * q_mesh[None, :]

    def potential(target):

        def add_source(source, summed):
            factor = coupling[target, source] * (local_weight + masses[target, source] / (k_squared + masses[target, source]))
            return summed + factor * spectra[source]
        summed = lax.fori_loop(0, qpoints, add_source, jnp.zeros_like(spectra[0]))
        return jnp.real(jnp.fft.ifftn(summed)).astype(jnp.float32)
    return lax.map(potential, q_nodes)
```

```python
import functools
import math

import jax
import jax.numpy as jnp
import numpy as np
from jax import lax
from jax.experimental import pallas as pl
from jax.experimental.pallas import tpu as pltpu
from jax.sharding import PartitionSpec as P

MESH = pl.DeviceIdType.MESH
F32 = jnp.float32
BF16 = jnp.bfloat16

NQ = 14
NX, NY, NZ = 128, 64, 512
CHUNKS = 2
QC = NQ // CHUNKS
KNOTS = NQ + 2
COLS = NY * NZ // NX
SUMS = 2 * NQ - 1

ZAB = 0.8491 / 9.0
Q_CUT = 5.0
STEP = 0.07
LOCAL = 0.25
LAM = math.sqrt(3.0) - 2.0


def frequencies(length):
    half = length // 2
    return np.array(list(range(half + 1)) + list(range(1, half)), dtype=np.float64)


def basis(length):
    half = length // 2
    points = np.arange(length)[:, None]
    waves = frequencies(length)[None, :]
    angle = 2.0 * np.pi / length * np.mod(points * waves, length)
    table = np.where(np.arange(length)[None, :] <= half, np.cos(angle), np.sin(angle))
    scale = np.full((1, length), math.sqrt(2.0 / length))
    scale[0, 0] = scale[0, half] = math.sqrt(1.0 / length)
    return table * scale


def halves(table):
    high = table.astype(BF16)
    low = (table - high.astype(np.float64)).astype(BF16)
    return high, low


def left_table(table):
    high, low = halves(table)
    return np.concatenate([high, high, low], axis=1)


def wave_squared(length):
    return (2.0 * np.pi / length * frequencies(length)) ** 2


def split(value):
    high = value.astype(BF16)
    return high, (value - high.astype(F32)).astype(BF16)


def left_multiply(table, value):
    high, low = split(value)
    return jnp.dot(table, jnp.concatenate([high, low, high], axis=0), preferred_element_type=F32)


def right_multiply(value, table_ref, transposed):
    high, low = split(value)
    rows = jnp.concatenate([high, low, high], axis=1)
    side = 1 if transposed else 0
    weights = jnp.concatenate([table_ref[0], table_ref[0], table_ref[1]], axis=side)
    return lax.dot_general(rows, weights, (((1,), (side,)), ((), ())), preferred_element_type=F32)


def kernel(
    sizes, dens, coup, tz, ty_f, ty_i, tx_f, tx_i, fx2, fz2, out,
    planes, q_buf, top_src, tops, thetas, mid, send1, recv1, spec, gain, prod, send2, recv2, send3,
    ssem, rsem,
):
    devices = NX
    nx, ny, nz = sizes
    group = ny * nz
    ix, iy, iz = lax.axis_index("gx"), lax.axis_index("gy"), lax.axis_index("gz")
    me = (ix * ny + iy) * nz + iz
    block_x, block_y, block_z = NX // nx, NY // ny, NZ // nz
    per_row = NZ // COLS

    def ids(p):
        return {"gx": p // group, "gy": (p // nz) % ny, "gz": p % nz}

    def send(src, dst, slot, p):
        pltpu.make_async_remote_copy(
            src, dst, ssem.at[slot], rsem.at[slot], device_id=ids(p), device_id_type=MESH
        ).start()

    def keep(src, dst, slot):
        pltpu.make_async_copy(src, dst, rsem.at[slot]).start()

    def received(ref, slot):
        pltpu.make_async_copy(ref, ref, rsem.at[slot]).wait()

    def sent(rows, slot):
        full, rest = divmod(rows, NX)
        if full:
            part = recv1.at[pl.ds(0, full)]
            pltpu.make_async_copy(part, part, ssem.at[slot]).wait()
        if rest // 8:
            part = recv1.at[0, pl.ds(0, rest // 8 * 8)]
            pltpu.make_async_copy(part, part, ssem.at[slot]).wait()
        for _ in range(rest % 8):
            part = recv1.at[0, 0]
            pltpu.make_async_copy(part, part, ssem.at[slot]).wait()

    barrier = pltpu.get_barrier_semaphore()

    def greet(d, carry):
        p = (me + d) % devices
        pl.semaphore_signal(barrier, inc=1, device_id=ids(p), device_id_type=MESH)
        return carry

    lax.fori_loop(1, devices, greet, 0)
    pl.semaphore_wait(barrier, devices - 1)

    here_y = pl.ds(pl.multiple_of(iy * block_y, 8), block_y)
    here_z = pl.ds(pl.multiple_of(iz * block_z, 128), block_z)
    for shift in range(5):

        def give(r, carry, shift=shift):
            row = (me + r * 5 + shift) % block_x
            p = (ix * block_x + row - (shift - 2) + devices) % devices
            src, dst = dens.at[row], planes.at[shift, here_y, here_z]

            @pl.when(p != me)
            def _():
                send(src, dst, 0, p)

            @pl.when(p == me)
            def _():
                keep(src, dst, 0)

            return carry

        lax.fori_loop(0, block_x, give, 0)
    received(planes, 0)

    own = planes[2]
    slope_x = (8.0 * (planes[3] - planes[1]) - (planes[4] - planes[0])) / 12.0
    grad_sq = slope_x * slope_x
    for axis, length in ((0, NY), (1, NZ)):
        nearer = pltpu.roll(own, length - 1, axis) - pltpu.roll(own, 1, axis)
        farther = pltpu.roll(own, length - 2, axis) - pltpu.roll(own, 2, axis)
        slope = (8.0 * nearer - farther) / 12.0
        grad_sq = grad_sq + slope * slope
    cube = (3.0 * math.pi * math.pi) * own
    fermi_k = jnp.exp(jnp.log(cube) / 3.0)
    fermi_k = fermi_k - (fermi_k - cube / (fermi_k * fermi_k)) * (1.0 / 3.0)
    reduced = grad_sq / (4.0 * fermi_k * fermi_k * own * own)
    scaled = fermi_k * (1.0 + ZAB * reduced) / Q_CUT
    series = jnp.full_like(scaled, 1.0 / 12.0)
    for order in range(11, 0, -1):
        series = series * scaled + 1.0 / order
    q_zero = Q_CUT * (1.0 - jnp.exp(-(series * scaled)))
    q_buf[...] = q_zero
    top = jnp.max(q_zero, axis=0, keepdims=True)
    top = jnp.broadcast_to(jnp.max(top, axis=1, keepdims=True), (1, 128))
    top_src[...] = top
    tops[me] = top

    def spread(d, carry):
        p = (me + d * 37) % devices
        send(top_src, tops.at[me], 1, p)
        return carry

    lax.fori_loop(1, devices, spread, 0)
    others = tops.at[pl.ds(0, devices - 1)]
    received(others, 1)
    q_top = jnp.max(tops[...])

    inv_top = 1.0 / jnp.broadcast_to(q_top, (8, 128))
    weight = math.sqrt(3.0) / 6.0

    def theta_rows(r, carry):
        rows = pl.ds(pl.multiple_of(r * 8, 8), 8)
        for lane in range(NZ // 128):
            lanes = pl.ds(lane * 128, 128)
            value = planes[2, rows, lanes] * weight
            position = jnp.maximum(
                (NQ - 1.0) + jnp.log(q_buf[rows, lanes] * inv_top) / STEP, 0.0
            )
            splines = []
            for j in range(-1, NQ + 1):
                offset = jnp.abs(position - float(j))
                wide = jnp.maximum(2.0 - offset, 0.0)
                narrow = jnp.maximum(1.0 - offset, 0.0)
                splines.append(wide * wide * wide - 4.0 * (narrow * narrow * narrow))
            up = [splines[0]]
            for j in range(1, KNOTS - 1):
                up.append(splines[j] + LAM * up[-1])
            down = splines[KNOTS - 1]
            for a in range(NQ - 1, -1, -1):
                below = LAM * down
                thetas[a, rows, lanes] = (up[a + 1] + below) * value
                down = splines[a + 1] + below
        return carry

    lax.fori_loop(0, NY // 8, theta_rows, 0)

    table_yf = ty_f[...]
    my_row, my_cols = me // per_row, pl.ds(pl.multiple_of((me % per_row) * COLS, 128), COLS)
    for c in range(CHUNKS):
        part = pl.ds(c * QC, QC)

        def y_forward(a, carry, c=c):
            mid[a] = left_multiply(table_yf, thetas[c * QC + a])
            return carry

        lax.fori_loop(0, QC, y_forward, 0)
        rows = right_multiply(mid[...].reshape(QC * NY, NZ), tz, False)
        send1[part] = rows.reshape(QC, NY, NZ)

        def lines_out(d, carry, c=c, part=part):
            p = (me + d * 37) % devices
            cols = pl.ds(pl.multiple_of((p % per_row) * COLS, 128), COLS)
            send(send1.at[part, p // per_row, cols], recv1.at[part, me], 2 + c, p)
            return carry

        lax.fori_loop(1, devices, lines_out, 0)
        keep(send1.at[part, my_row, my_cols], recv1.at[part, me], 2 + c)

    wave_y = jnp.where(my_row <= NY // 2, my_row, my_row - NY // 2).astype(F32) * (2.0 * math.pi / NY)
    yz2 = fz2[:, my_cols] + wave_y * wave_y
    top_sq = jnp.broadcast_to(q_top * q_top, (8, COLS))

    def gain_rows(r, carry):
        rows = pl.ds(pl.multiple_of(r * 8, 8), 8)
        line = fx2[rows, :]
        k_sq = jnp.concatenate([line] * (COLS // 128), axis=1) + yz2
        for s in range(SUMS):
            mass = top_sq * math.exp(-STEP * (2 * NQ - 2 - s))
            gain[s, rows, :] = LOCAL + mass / (k_sq + mass)
        return carry

    lax.fori_loop(0, NX // 8, gain_rows, 0)

    table_xf, table_xi = tx_f[...], tx_i[...]
    for c in range(CHUNKS):
        received(recv1.at[pl.ds(c * QC, QC)], 2 + c)

        def x_forward(a, carry, c=c):
            spec[c * QC + a] = left_multiply(table_xf, recv1[c * QC + a])
            return carry

        lax.fori_loop(0, QC, x_forward, 0)

    for c in range(CHUNKS):
        part = pl.ds(c * QC, QC)

        def couple(r, carry, c=c):
            rows = pl.ds(pl.multiple_of(r * 8, 8), 8)
            for lane in range(COLS // 128):
                lanes = pl.ds(lane * 128, 128)
                source = [spec[b, rows, lanes] for b in range(NQ)]
                factor = {}
                for s in range(c * QC, c * QC + QC + NQ - 1):
                    factor[s] = gain[s, rows, lanes]
                for a in range(QC):
                    total = None
                    for b in range(NQ):
                        term = (coup[c * QC + a, b] * factor[c * QC + a + b]) * source[b]
                        total = term if total is None else total + term
                    prod[a, rows, lanes] = total
            return carry

        lax.fori_loop(0, NX // 8, couple, 0)

        def x_inverse(a, carry, c=c):
            send2[c * QC + a] = left_multiply(table_xi, prod[a])
            return carry

        lax.fori_loop(0, QC, x_inverse, 0)

        def lines_back(d, carry, c=c, part=part):
            p = (me + d * 37) % devices
            send(send2.at[part, p], recv2.at[part, my_row, my_cols], 4 + c, p)
            return carry

        lax.fori_loop(1, devices, lines_back, 0)
        keep(send2.at[part, me], recv2.at[part, my_row, my_cols], 4 + c)

    table_yi = ty_i[...]
    here = me % group
    row_x = me % block_x
    for c in range(CHUNKS):
        part = pl.ds(c * QC, QC)
        received(recv2.at[part], 4 + c)
        rows = right_multiply(recv2[part].reshape(QC * NY, NZ), tz, True)
        mid[...] = rows.reshape(QC, NY, NZ)

        def y_inverse(a, carry, c=c):
            send3[c * QC + a] = left_multiply(table_yi, mid[a])
            return carry

        lax.fori_loop(0, QC, y_inverse, 0)

        def block(w):
            ys = pl.ds(pl.multiple_of((w // nz) * block_y, 8), block_y)
            zs = pl.ds(pl.multiple_of((w % nz) * block_z, 128), block_z)
            return send3.at[part, ys, zs]

        def blocks_out(d, carry, c=c, part=part, block=block):
            w = (here + d * 11) % group
            send(block(w), out.at[part, row_x], 6 + c, ix * group + w)
            return carry

        lax.fori_loop(1, group, blocks_out, 0)
        keep(block(here), out.at[part, row_x], 6 + c)

    for c in range(CHUNKS):
        received(out.at[pl.ds(c * QC, QC)], 6 + c)

    sent((5 * block_x - 5) * block_y * block_z // COLS, 0)

    def sent_block(i, carry):
        part = dens.at[0]
        pltpu.make_async_copy(part, part, ssem.at[0]).wait()
        return carry

    edge = jnp.maximum(2 - row_x, 0) + jnp.maximum(row_x - (block_x - 3), 0)
    lax.fori_loop(0, edge, sent_block, 0)
    pltpu.make_async_copy(others, others, ssem.at[1]).wait()
    for c in range(CHUNKS):
        sent((devices - 1) * QC, 2 + c)
        sent((devices - 1) * QC, 4 + c)
        sent((group - 1) * QC * block_y * block_z // COLS, 6 + c)


def solution(mesh):
    sizes = tuple(mesh.shape[axis] for axis in ("gx", "gy", "gz"))
    bz = basis(NZ)
    tz = np.stack(halves(bz))
    by, bx = basis(NY), basis(NX)
    fx2 = np.broadcast_to(wave_squared(NX)[:, None], (NX, 128)).astype(np.float32)
    fz2 = np.broadcast_to(wave_squared(NZ)[None, :], (8, NZ)).astype(np.float32)
    tables = (tz, left_table(by.T), left_table(by), left_table(bx.T), left_table(bx), fx2, fz2)

    def body(density, coupling):
        vmem = pl.BlockSpec(memory_space=pltpu.VMEM)
        block = density.shape
        return pl.pallas_call(
            functools.partial(kernel, sizes),
            out_shape=jax.ShapeDtypeStruct((NQ,) + block, F32),
            in_specs=[vmem, pl.BlockSpec(memory_space=pltpu.SMEM)] + [vmem] * len(tables),
            out_specs=vmem,
            scratch_shapes=[
                pltpu.VMEM((5, NY, NZ), F32),
                pltpu.VMEM((NY, NZ), F32),
                pltpu.VMEM((1, 128), F32),
                pltpu.VMEM((NX, 1, 128), F32),
                pltpu.VMEM((NQ, NY, NZ), F32),
                pltpu.VMEM((QC, NY, NZ), F32),
                pltpu.VMEM((NQ, NY, NZ), F32),
                pltpu.VMEM((NQ, NX, COLS), F32),
                pltpu.VMEM((NQ, NX, COLS), F32),
                pltpu.VMEM((SUMS, NX, COLS), F32),
                pltpu.VMEM((QC, NX, COLS), F32),
                pltpu.VMEM((NQ, NX, COLS), F32),
                pltpu.VMEM((NQ, NY, NZ), F32),
                pltpu.VMEM((NQ, NY, NZ), F32),
                pltpu.SemaphoreType.DMA((8,)),
                pltpu.SemaphoreType.DMA((8,)),
            ],
            compiler_params=pltpu.CompilerParams(
                collective_id=0, has_side_effects=True, vmem_limit_bytes=56 * 1024 * 1024
            ),
            name="convolve",
        )(density, coupling, *[jnp.asarray(t) for t in tables])

    placed = (P("gx", "gy", "gz"), P())
    return jax.shard_map(
        body, mesh=mesh, in_specs=placed, out_specs=P(None, "gx", "gy", "gz"), check_vma=False
    )
```

```python
import functools
import math

import jax
import jax.numpy as jnp
import numpy as np
from jax import lax
from jax.experimental import pallas as pl
from jax.experimental.pallas import tpu as pltpu
from jax.sharding import PartitionSpec as P

MESH = pl.DeviceIdType.MESH
F32 = jnp.float32
BF16 = jnp.bfloat16

NQ = 14
NX, NY, NZ = 128, 64, 512
CHUNKS = 2
QC = NQ // CHUNKS
KNOTS = NQ + 2
COLS = NY * NZ // NX
SUMS = 2 * NQ - 1

ZAB = 0.8491 / 9.0
Q_CUT = 5.0
STEP = 0.07
LOCAL = 0.25
LAM = math.sqrt(3.0) - 2.0


def frequencies(length):
    half = length // 2
    return np.array(list(range(half + 1)) + list(range(1, half)), dtype=np.float64)


def basis(length):
    half = length // 2
    points = np.arange(length)[:, None]
    waves = frequencies(length)[None, :]
    angle = 2.0 * np.pi / length * np.mod(points * waves, length)
    table = np.where(np.arange(length)[None, :] <= half, np.cos(angle), np.sin(angle))
    scale = np.full((1, length), math.sqrt(2.0 / length))
    scale[0, 0] = scale[0, half] = math.sqrt(1.0 / length)
    return table * scale


def halves(table):
    high = table.astype(BF16)
    low = (table - high.astype(np.float64)).astype(BF16)
    return high, low


def left_table(table):
    high, low = halves(table)
    return np.concatenate([high, high, low], axis=1)


def wave_squared(length):
    return (2.0 * np.pi / length * frequencies(length)) ** 2


def split(value):
    high = value.astype(BF16)
    return high, (value - high.astype(F32)).astype(BF16)


def left_multiply(table, value):
    high, low = split(value)
    return jnp.dot(table, jnp.concatenate([high, low, high], axis=0), preferred_element_type=F32)


def right_multiply(value, table_ref, transposed):
    high, low = split(value)
    rows = jnp.concatenate([high, low, high], axis=1)
    side = 1 if transposed else 0
    weights = jnp.concatenate([table_ref[0], table_ref[0], table_ref[1]], axis=side)
    return lax.dot_general(rows, weights, (((1,), (side,)), ((), ())), preferred_element_type=F32)


def kernel(
    sizes, dens, coup, tz, ty_f, ty_i, tx_f, tx_i, fx2, fz2, out,
    planes, q_buf, top_src, tops, thetas, mid, send1, recv1, spec, gain, prod, send2, recv2, send3,
    ssem, rsem,
):
    devices = NX
    nx, ny, nz = sizes
    group = ny * nz
    ix, iy, iz = lax.axis_index("gx"), lax.axis_index("gy"), lax.axis_index("gz")
    me = (ix * ny + iy) * nz + iz
    block_x, block_y, block_z = NX // nx, NY // ny, NZ // nz
    per_row = NZ // COLS

    def ids(p):
        rest = lax.rem(p, group)
        return {"gx": lax.div(p, group), "gy": lax.div(rest, nz), "gz": lax.rem(rest, nz)}

    def send(src, dst, slot, p):
        pltpu.make_async_remote_copy(
            src, dst, ssem.at[slot], rsem.at[slot], device_id=ids(p), device_id_type=MESH
        ).start()

    def keep(src, dst, slot):
        pltpu.make_async_copy(src, dst, rsem.at[slot]).start()

    def received(ref, slot):
        pltpu.make_async_copy(ref, ref, rsem.at[slot]).wait()

    def sent(rows, slot):
        full, rest = divmod(rows, NX)
        if full:
            part = recv1.at[pl.ds(0, full)]
            pltpu.make_async_copy(part, part, ssem.at[slot]).wait()
        if rest // 8:
            part = recv1.at[0, pl.ds(0, rest // 8 * 8)]
            pltpu.make_async_copy(part, part, ssem.at[slot]).wait()
        for _ in range(rest % 8):
            part = recv1.at[0, 0]
            pltpu.make_async_copy(part, part, ssem.at[slot]).wait()

    barrier = pltpu.get_barrier_semaphore()

    def greet(d, carry):
        p = lax.rem(me + d, devices)
        pl.semaphore_signal(barrier, inc=1, device_id=ids(p), device_id_type=MESH)
        return carry

    lax.fori_loop(1, devices, greet, 0)
    pl.semaphore_wait(barrier, devices - 1)

    here_y = pl.ds(pl.multiple_of(iy * block_y, 8), block_y)
    here_z = pl.ds(pl.multiple_of(iz * block_z, 128), block_z)
    for shift in range(5):

        def give(r, carry, shift=shift):
            row = lax.rem(me + r * 5 + shift, block_x)
            p = lax.rem(ix * block_x + row - (shift - 2) + devices, devices)
            src, dst = dens.at[row], planes.at[shift, here_y, here_z]

            @pl.when(p != me)
            def _():
                send(src, dst, 0, p)

            @pl.when(p == me)
            def _():
                keep(src, dst, 0)

            return carry

        lax.fori_loop(0, block_x, give, 0)
    received(planes, 0)

    own = planes[2]
    slope_x = (8.0 * (planes[3] - planes[1]) - (planes[4] - planes[0])) / 12.0
    grad_sq = slope_x * slope_x
    for axis, length in ((0, NY), (1, NZ)):
        nearer = pltpu.roll(own, length - 1, axis) - pltpu.roll(own, 1, axis)
        farther = pltpu.roll(own, length - 2, axis) - pltpu.roll(own, 2, axis)
        slope = (8.0 * nearer - farther) / 12.0
        grad_sq = grad_sq + slope * slope
    cube = (3.0 * math.pi * math.pi) * own
    fermi_k = jnp.exp(jnp.log(cube) / 3.0)
    fermi_k = fermi_k - (fermi_k - cube / (fermi_k * fermi_k)) * (1.0 / 3.0)
    reduced = grad_sq / (4.0 * fermi_k * fermi_k * own * own)
    scaled = fermi_k * (1.0 + ZAB * reduced) / Q_CUT
    series = jnp.full_like(scaled, 1.0 / 12.0)
    for order in range(11, 0, -1):
        series = series * scaled + 1.0 / order
    q_zero = Q_CUT * (1.0 - jnp.exp(-(series * scaled)))
    q_buf[...] = q_zero
    top = jnp.max(q_zero, axis=0, keepdims=True)
    top = jnp.broadcast_to(jnp.max(top, axis=1, keepdims=True), (1, 128))
    top_src[...] = top
    tops[me] = top

    def spread(d, carry):
        p = lax.rem(me + d * 37, devices)
        send(top_src, tops.at[me], 1, p)
        return carry

    lax.fori_loop(1, devices, spread, 0)
    others = tops.at[pl.ds(0, devices - 1)]
    received(others, 1)
    q_top = jnp.max(tops[...])

    inv_top = 1.0 / jnp.broadcast_to(q_top, (8, 128))
    weight = math.sqrt(3.0) / 6.0

    def theta_rows(r, carry):
        rows = pl.ds(pl.multiple_of(r * 8, 8), 8)
        for lane in range(NZ // 128):
            lanes = pl.ds(lane * 128, 128)
            value = planes[2, rows, lanes] * weight
            position = jnp.maximum(
                (NQ - 1.0) + jnp.log(q_buf[rows, lanes] * inv_top) / STEP, 0.0
            )
            splines = []
            for j in range(-1, NQ + 1):
                offset = jnp.abs(position - float(j))
                wide = jnp.maximum(2.0 - offset, 0.0)
                narrow = jnp.maximum(1.0 - offset, 0.0)
                splines.append(wide * wide * wide - 4.0 * (narrow * narrow * narrow))
            up = [splines[0]]
            for j in range(1, KNOTS - 1):
                up.append(splines[j] + LAM * up[-1])
            down = splines[KNOTS - 1]
            for a in range(NQ - 1, -1, -1):
                below = LAM * down
                thetas[a, rows, lanes] = (up[a + 1] + below) * value
                down = splines[a + 1] + below
        return carry

    lax.fori_loop(0, NY // 8, theta_rows, 0)

    table_yf = ty_f[...]
    my_row, my_cols = lax.div(me, per_row), pl.ds(pl.multiple_of(lax.rem(me, per_row) * COLS, 128), COLS)
    for c in range(CHUNKS):
        part = pl.ds(c * QC, QC)

        def y_forward(a, carry, c=c):
            mid[a] = left_multiply(table_yf, thetas[c * QC + a])
            return carry

        lax.fori_loop(0, QC, y_forward, 0)
        rows = right_multiply(mid[...].reshape(QC * NY, NZ), tz, False)
        send1[part] = rows.reshape(QC, NY, NZ)

        def lines_out(d, carry, c=c, part=part):
            p = lax.rem(me + d * 37, devices)
            cols = pl.ds(pl.multiple_of(lax.rem(p, per_row) * COLS, 128), COLS)
            send(send1.at[part, lax.div(p, per_row), cols], recv1.at[part, me], 2 + c, p)
            return carry

        lax.fori_loop(1, devices, lines_out, 0)
        keep(send1.at[part, my_row, my_cols], recv1.at[part, me], 2 + c)

    wave_y = jnp.where(my_row <= NY // 2, my_row, my_row - NY // 2).astype(F32) * (2.0 * math.pi / NY)
    yz2 = fz2[:, my_cols] + wave_y * wave_y
    top_sq = jnp.broadcast_to(q_top * q_top, (8, COLS))

    def gain_rows(r, carry):
        rows = pl.ds(pl.multiple_of(r * 8, 8), 8)
        line = fx2[rows, :]
        k_sq = jnp.concatenate([line] * (COLS // 128), axis=1) + yz2
        for s in range(SUMS):
            mass = top_sq * math.exp(-STEP * (2 * NQ - 2 - s))
            gain[s, rows, :] = LOCAL + mass / (k_sq + mass)
        return carry

    lax.fori_loop(0, NX // 8, gain_rows, 0)

    table_xf, table_xi = tx_f[...], tx_i[...]
    for c in range(CHUNKS):
        received(recv1.at[pl.ds(c * QC, QC)], 2 + c)

        def x_forward(a, carry, c=c):
            spec[c * QC + a] = left_multiply(table_xf, recv1[c * QC + a])
            return carry

        lax.fori_loop(0, QC, x_forward, 0)

    for c in range(CHUNKS):
        part = pl.ds(c * QC, QC)

        def couple(r, carry, c=c):
            rows = pl.ds(pl.multiple_of(r * 8, 8), 8)
            for lane in range(COLS // 128):
                lanes = pl.ds(lane * 128, 128)
                source = [spec[b, rows, lanes] for b in range(NQ)]
                factor = {}
                for s in range(c * QC, c * QC + QC + NQ - 1):
                    factor[s] = gain[s, rows, lanes]
                for a in range(QC):
                    total = None
                    for b in range(NQ):
                        term = (coup[c * QC + a, b] * factor[c * QC + a + b]) * source[b]
                        total = term if total is None else total + term
                    prod[a, rows, lanes] = total
            return carry

        lax.fori_loop(0, NX // 8, couple, 0)

        def x_inverse(a, carry, c=c):
            send2[c * QC + a] = left_multiply(table_xi, prod[a])
            return carry

        lax.fori_loop(0, QC, x_inverse, 0)

        def lines_back(d, carry, c=c, part=part):
            p = lax.rem(me + d * 37, devices)
            send(send2.at[part, p], recv2.at[part, my_row, my_cols], 4 + c, p)
            return carry

        lax.fori_loop(1, devices, lines_back, 0)
        keep(send2.at[part, me], recv2.at[part, my_row, my_cols], 4 + c)

    table_yi = ty_i[...]
    here = lax.rem(me, group)
    row_x = lax.rem(me, block_x)
    for c in range(CHUNKS):
        part = pl.ds(c * QC, QC)
        received(recv2.at[part], 4 + c)
        rows = right_multiply(recv2[part].reshape(QC * NY, NZ), tz, True)
        mid[...] = rows.reshape(QC, NY, NZ)

        def y_inverse(a, carry, c=c):
            send3[c * QC + a] = left_multiply(table_yi, mid[a])
            return carry

        lax.fori_loop(0, QC, y_inverse, 0)

        def block(w):
            ys = pl.ds(pl.multiple_of(lax.div(w, nz) * block_y, 8), block_y)
            zs = pl.ds(pl.multiple_of(lax.rem(w, nz) * block_z, 128), block_z)
            return send3.at[part, ys, zs]

        def blocks_out(d, carry, c=c, part=part, block=block):
            w = lax.rem(here + d * 11, group)
            send(block(w), out.at[part, row_x], 6 + c, ix * group + w)
            return carry

        lax.fori_loop(1, group, blocks_out, 0)
        keep(block(here), out.at[part, row_x], 6 + c)

    for c in range(CHUNKS):
        received(out.at[pl.ds(c * QC, QC)], 6 + c)

    sent((5 * block_x - 5) * block_y * block_z // COLS, 0)

    def sent_block(i, carry):
        part = dens.at[0]
        pltpu.make_async_copy(part, part, ssem.at[0]).wait()
        return carry

    edge = jnp.maximum(2 - row_x, 0) + jnp.maximum(row_x - (block_x - 3), 0)
    lax.fori_loop(0, edge, sent_block, 0)
    pltpu.make_async_copy(others, others, ssem.at[1]).wait()
    for c in range(CHUNKS):
        sent((devices - 1) * QC, 2 + c)
        sent((devices - 1) * QC, 4 + c)
        sent((group - 1) * QC * block_y * block_z // COLS, 6 + c)


def solution(mesh):
    sizes = tuple(mesh.shape[axis] for axis in ("gx", "gy", "gz"))
    bz = basis(NZ)
    tz = np.stack(halves(bz))
    by, bx = basis(NY), basis(NX)
    fx2 = np.broadcast_to(wave_squared(NX)[:, None], (NX, 128)).astype(np.float32)
    fz2 = np.broadcast_to(wave_squared(NZ)[None, :], (8, NZ)).astype(np.float32)
    tables = (tz, left_table(by.T), left_table(by), left_table(bx.T), left_table(bx), fx2, fz2)

    def body(density, coupling):
        vmem = pl.BlockSpec(memory_space=pltpu.VMEM)
        block = density.shape
        return pl.pallas_call(
            functools.partial(kernel, sizes),
            out_shape=jax.ShapeDtypeStruct((NQ,) + block, F32),
            in_specs=[vmem, pl.BlockSpec(memory_space=pltpu.SMEM)] + [vmem] * len(tables),
            out_specs=vmem,
            scratch_shapes=[
                pltpu.VMEM((5, NY, NZ), F32),
                pltpu.VMEM((NY, NZ), F32),
                pltpu.VMEM((1, 128), F32),
                pltpu.VMEM((NX, 1, 128), F32),
                pltpu.VMEM((NQ, NY, NZ), F32),
                pltpu.VMEM((QC, NY, NZ), F32),
                pltpu.VMEM((NQ, NY, NZ), F32),
                pltpu.VMEM((NQ, NX, COLS), F32),
                pltpu.VMEM((NQ, NX, COLS), F32),
                pltpu.VMEM((SUMS, NX, COLS), F32),
                pltpu.VMEM((QC, NX, COLS), F32),
                pltpu.VMEM((NQ, NX, COLS), F32),
                pltpu.VMEM((NQ, NY, NZ), F32),
                pltpu.VMEM((NQ, NY, NZ), F32),
                pltpu.SemaphoreType.DMA((8,)),
                pltpu.SemaphoreType.DMA((8,)),
            ],
            compiler_params=pltpu.CompilerParams(
                collective_id=0, has_side_effects=True, vmem_limit_bytes=56 * 1024 * 1024
            ),
            name="convolve",
        )(density, coupling, *[jnp.asarray(t) for t in tables])

    placed = (P("gx", "gy", "gz"), P())
    return jax.shard_map(
        body, mesh=mesh, in_specs=placed, out_specs=P(None, "gx", "gy", "gz"), check_vma=False
    )
```

```python
import functools
import math

import jax
import jax.numpy as jnp
import numpy as np
from jax import lax
from jax.experimental import pallas as pl
from jax.experimental.pallas import tpu as pltpu
from jax.sharding import PartitionSpec as P

MESH = pl.DeviceIdType.MESH
F32 = jnp.float32
BF16 = jnp.bfloat16

NQ = 14
NX, NY, NZ = 128, 64, 512
CHUNKS = 2
QC = NQ // CHUNKS
KNOTS = NQ + 2
COLS = NY * NZ // NX
SUMS = 2 * NQ - 1

ZAB = 0.8491 / 9.0
Q_CUT = 5.0
STEP = 0.07
LOCAL = 0.25
LAM = math.sqrt(3.0) - 2.0


def frequencies(length):
    half = length // 2
    return np.array(list(range(half + 1)) + list(range(1, half)), dtype=np.float64)


def basis(length):
    half = length // 2
    points = np.arange(length)[:, None]
    waves = frequencies(length)[None, :]
    angle = 2.0 * np.pi / length * np.mod(points * waves, length)
    table = np.where(np.arange(length)[None, :] <= half, np.cos(angle), np.sin(angle))
    scale = np.full((1, length), math.sqrt(2.0 / length))
    scale[0, 0] = scale[0, half] = math.sqrt(1.0 / length)
    return table * scale


def halves(table):
    high = table.astype(BF16)
    low = (table - high.astype(np.float64)).astype(BF16)
    return high, low


def left_table(table):
    high, low = halves(table)
    return np.concatenate([high, high, low], axis=1)


def wave_squared(length):
    return (2.0 * np.pi / length * frequencies(length)) ** 2


def split(value):
    high = value.astype(BF16)
    return high, (value - high.astype(F32)).astype(BF16)


def left_multiply(table, value):
    high, low = split(value)
    return jnp.dot(table, jnp.concatenate([high, low, high], axis=0), preferred_element_type=F32)


def right_multiply(value, table_ref, transposed):
    high, low = split(value)
    rows = jnp.concatenate([high, low, high], axis=1)
    side = 1 if transposed else 0
    weights = jnp.concatenate([table_ref[0], table_ref[0], table_ref[1]], axis=side)
    return lax.dot_general(rows, weights, (((1,), (side,)), ((), ())), preferred_element_type=F32)


def kernel(
    sizes, dens, coup, tz, ty_f, ty_i, tx_f, tx_i, fx2, fz2, out,
    ext, zext, zsend, zhalo, planes, q_buf, top_src, near_tops, far_tops, thetas, mid, send1, recv1, spec, gain, prod, send2, recv2, send3,
    ssem, rsem, hsend, hrecv,
):
    devices = NX
    nx, ny, nz = sizes
    group = ny * nz
    ix, iy, iz = lax.axis_index("gx"), lax.axis_index("gy"), lax.axis_index("gz")
    me = (ix * ny + iy) * nz + iz
    block_x, block_y, block_z = NX // nx, NY // ny, NZ // nz
    per_row = NZ // COLS

    def send(src, dst, slot, to):
        pltpu.make_async_remote_copy(
            src, dst, ssem.at[slot], rsem.at[slot], device_id=to, device_id_type=MESH
        ).start()

    def keep(src, dst, slot):
        pltpu.make_async_copy(src, dst, rsem.at[slot]).start()

    def received(ref, slot):
        pltpu.make_async_copy(ref, ref, rsem.at[slot]).wait()

    def sent(rows, slot):
        full, rest = divmod(rows, NX)
        if full:
            part = recv1.at[pl.ds(0, full)]
            pltpu.make_async_copy(part, part, ssem.at[slot]).wait()
        if rest // 8:
            part = recv1.at[0, pl.ds(0, rest // 8 * 8)]
            pltpu.make_async_copy(part, part, ssem.at[slot]).wait()
        for _ in range(rest % 8):
            part = recv1.at[0, 0]
            pltpu.make_async_copy(part, part, ssem.at[slot]).wait()

    block = dens[...]
    ext[pl.ds(2, block_x), pl.ds(8, block_y), :] = block
    turned = block.reshape(block_x * block_y, block_z).T
    zext[pl.ds(8, block_z), :] = turned
    zsend[0] = turned[:2]
    zsend[1] = turned[block_z - 2 :]

    gys = [lax.rem(iy + j, ny) for j in range(ny)]
    gzs = [lax.rem(iz + j, nz) for j in range(nz)]
    near = [(dy, dz) for dz in range(nz) for dy in range(ny)]
    barrier = pltpu.get_barrier_semaphore()
    for dy, dz in near[1:]:
        pl.semaphore_signal(
            barrier, inc=1, device_id={"gy": gys[dy], "gz": gzs[dz]}, device_id_type=MESH
        )
    for dx in range(1, nx):
        pl.semaphore_signal(
            barrier, inc=1, device_id={"gx": lax.rem(ix + dx, nx)}, device_id_type=MESH
        )
    pl.semaphore_wait(barrier, group - 1 + nx - 1)

    halos = []

    def halo(src, dst, to):
        slot = len(halos)
        copy = pltpu.make_async_remote_copy(
            src, dst, hsend.at[slot], hrecv.at[slot], device_id=to, device_id_type=MESH
        )
        copy.start()
        halos.append(copy)

    low_x, high_x = {"gx": lax.rem(ix + nx - 1, nx)}, {"gx": lax.rem(ix + 1, nx)}
    low_y, high_y = {"gy": gys[ny - 1]}, {"gy": gys[1]}
    low_z, high_z = {"gz": gzs[nz - 1]}, {"gz": gzs[1]}
    inner_x, inner_y = pl.ds(2, block_x), pl.ds(8, block_y)
    halo(dens.at[pl.ds(0, 2)], ext.at[pl.ds(block_x + 2, 2), inner_y], low_x)
    halo(dens.at[pl.ds(block_x - 2, 2)], ext.at[pl.ds(0, 2), inner_y], high_x)
    for k in range(2):
        halo(dens.at[:, k, :], ext.at[inner_x, block_y + 8 + k, :], low_y)
        halo(dens.at[:, block_y - 2 + k, :], ext.at[inner_x, 6 + k, :], high_y)
    halo(zsend.at[0], zhalo.at[1], low_z)
    halo(zsend.at[1], zhalo.at[0], high_z)

    here, row_x = iy * nz + iz, iy * nz + iz
    here_y = pl.ds(pl.multiple_of(iy * block_y, 8), block_y)
    here_z = pl.ds(pl.multiple_of(iz * block_z, 128), block_z)

    def rows_out(src, which):
        for dy, dz in near:
            row = gys[dy] * nz + gzs[dz]
            dst = planes.at[which, here_y, here_z]
            if dy or dz:
                send(src.at[row], dst, 0, {"gy": gys[dy], "gz": gzs[dz]})
            else:
                keep(src.at[row], dst, 0)

    rows_out(dens, 0)
    for copy in halos:
        copy.wait()

    zext[6:8, :] = zhalo[0]
    zext[pl.ds(block_z + 8, 2), :] = zhalo[1]

    def squared_slope(at):
        slope = (8.0 * (at(1) - at(-1)) - (at(2) - at(-2))) / 12.0
        return slope * slope

    grad_sq = squared_slope(lambda o: ext[pl.ds(2 + o, block_x), inner_y, :])
    grad_sq = grad_sq + squared_slope(lambda o: ext[inner_x, pl.ds(8 + o, block_y), :])
    along_z = squared_slope(lambda o: zext[pl.ds(8 + o, block_z), :])
    grad_sq = grad_sq + along_z.T.reshape(block_x, block_y, block_z)
    cube = (3.0 * math.pi * math.pi) * block
    fermi_k = jnp.exp(jnp.log(cube) / 3.0)
    fermi_k = fermi_k - (fermi_k - cube / (fermi_k * fermi_k)) * (1.0 / 3.0)
    reduced = grad_sq / (4.0 * fermi_k * fermi_k * block * block)
    scaled = fermi_k * (1.0 + ZAB * reduced) / Q_CUT
    series = jnp.full_like(scaled, 1.0 / 12.0)
    for order in range(11, 0, -1):
        series = series * scaled + 1.0 / order
    q_zero = Q_CUT * (1.0 - jnp.exp(-(series * scaled)))
    q_buf[...] = q_zero
    top = jnp.max(jnp.max(q_zero, axis=0), axis=0, keepdims=True)
    top = jnp.broadcast_to(jnp.max(top, axis=1, keepdims=True), (1, 128))
    top_src[0] = top
    near_tops[here] = top

    for dy, dz in near[1:]:
        send(top_src.at[0], near_tops.at[here], 1, {"gy": gys[dy], "gz": gzs[dz]})
    rows_out(q_buf, 1)
    others = near_tops.at[pl.ds(0, group - 1)]
    received(others, 1)
    top = jnp.max(near_tops[...], axis=0)
    top_src[1] = top
    far_tops[ix] = top
    for dx in range(1, nx):
        send(top_src.at[1], far_tops.at[ix], 8, {"gx": lax.rem(ix + dx, nx)})
    far_others = far_tops.at[pl.ds(0, nx - 1)]
    received(far_others, 8)
    q_top = jnp.max(far_tops[...])
    received(planes, 0)

    inv_top = 1.0 / jnp.broadcast_to(q_top, (8, 128))
    weight = math.sqrt(3.0) / 6.0

    def theta_rows(r, carry):
        rows = pl.ds(pl.multiple_of(r * 8, 8), 8)
        for lane in range(NZ // 128):
            lanes = pl.ds(lane * 128, 128)
            value = planes[0, rows, lanes] * weight
            position = jnp.maximum(
                (NQ - 1.0) + jnp.log(planes[1, rows, lanes] * inv_top) / STEP, 0.0
            )
            splines = []
            for j in range(-1, NQ + 1):
                offset = jnp.abs(position - float(j))
                wide = jnp.maximum(2.0 - offset, 0.0)
                narrow = jnp.maximum(1.0 - offset, 0.0)
                splines.append(wide * wide * wide - 4.0 * (narrow * narrow * narrow))
            up = [splines[0]]
            for j in range(1, KNOTS - 1):
                up.append(splines[j] + LAM * up[-1])
            down = splines[KNOTS - 1]
            for a in range(NQ - 1, -1, -1):
                below = LAM * down
                thetas[a, rows, lanes] = (up[a + 1] + below) * value
                down = splines[a + 1] + below
        return carry

    lax.fori_loop(0, NY // 8, theta_rows, 0)

    table_yf = ty_f[...]
    rows_of = [lax.div(g, per_row) for g in gzs]
    cols_of = [pl.ds(pl.multiple_of(lax.rem(g, per_row) * COLS, 128), COLS) for g in gzs]
    spread = [near[(m * 7) % group] for m in range(group)]

    def to_all(issue):
        def step(t, carry):
            for m, (dy, dz) in enumerate(spread):
                gx = lax.rem(ix + t + 3 * m, nx)
                p = (gx * ny + gys[dy]) * nz + gzs[dz]
                row = (gx * ny + gys[dy]) * (nz // per_row) + rows_of[dz]
                to = {"gx": gx, "gy": gys[dy], "gz": gzs[dz]}
                run = functools.partial(issue, p, row, cols_of[dz], to)
                if dy or dz:
                    run()
                else:
                    pl.when(t != (nx - 3 * m) % nx)(run)
            return carry

        lax.fori_loop(0, nx, step, 0)

    my_row, my_cols = lax.div(me, per_row), pl.ds(pl.multiple_of(lax.rem(me, per_row) * COLS, 128), COLS)
    for c in range(CHUNKS):
        part = pl.ds(c * QC, QC)

        def y_forward(a, carry, c=c):
            mid[a] = left_multiply(table_yf, thetas[c * QC + a])
            return carry

        lax.fori_loop(0, QC, y_forward, 0)
        rows = right_multiply(mid[...].reshape(QC * NY, NZ), tz, False)
        send1[part] = rows.reshape(QC, NY, NZ)

        to_all(lambda p, row, cols, to: send(send1.at[part, row, cols], recv1.at[part, me], 2 + c, to))
        keep(send1.at[part, my_row, my_cols], recv1.at[part, me], 2 + c)

    wave_y = jnp.where(my_row <= NY // 2, my_row, my_row - NY // 2).astype(F32) * (2.0 * math.pi / NY)
    yz2 = fz2[:, my_cols] + wave_y * wave_y
    top_sq = jnp.broadcast_to(q_top * q_top, (8, COLS))

    def gain_rows(r, carry):
        rows = pl.ds(pl.multiple_of(r * 8, 8), 8)
        line = fx2[rows, :]
        k_sq = jnp.concatenate([line] * (COLS // 128), axis=1) + yz2
        for s in range(SUMS):
            mass = top_sq * math.exp(-STEP * (2 * NQ - 2 - s))
            gain[s, rows, :] = LOCAL + mass / (k_sq + mass)
        return carry

    lax.fori_loop(0, NX // 8, gain_rows, 0)

    table_xf, table_xi = tx_f[...], tx_i[...]
    for c in range(CHUNKS):
        received(recv1.at[pl.ds(c * QC, QC)], 2 + c)

        def x_forward(a, carry, c=c):
            spec[c * QC + a] = left_multiply(table_xf, recv1[c * QC + a])
            return carry

        lax.fori_loop(0, QC, x_forward, 0)

    for c in range(CHUNKS):
        part = pl.ds(c * QC, QC)

        def couple(r, carry, c=c):
            rows = pl.ds(pl.multiple_of(r * 8, 8), 8)
            for lane in range(COLS // 128):
                lanes = pl.ds(lane * 128, 128)
                source = [spec[b, rows, lanes] for b in range(NQ)]
                factor = {}
                for s in range(c * QC, c * QC + QC + NQ - 1):
                    factor[s] = gain[s, rows, lanes]
                for a in range(QC):
                    total = None
                    for b in range(NQ):
                        term = (coup[c * QC + a, b] * factor[c * QC + a + b]) * source[b]
                        total = term if total is None else total + term
                    prod[a, rows, lanes] = total
            return carry

        lax.fori_loop(0, NX // 8, couple, 0)

        def x_inverse(a, carry, c=c):
            send2[c * QC + a] = left_multiply(table_xi, prod[a])
            return carry

        lax.fori_loop(0, QC, x_inverse, 0)

        to_all(lambda p, row, cols, to: send(send2.at[part, p], recv2.at[part, my_row, my_cols], 4 + c, to))
        keep(send2.at[part, me], recv2.at[part, my_row, my_cols], 4 + c)

    table_yi = ty_i[...]
    for c in range(CHUNKS):
        part = pl.ds(c * QC, QC)
        received(recv2.at[part], 4 + c)
        rows = right_multiply(recv2[part].reshape(QC * NY, NZ), tz, True)
        mid[...] = rows.reshape(QC, NY, NZ)

        def y_inverse(a, carry, c=c):
            send3[c * QC + a] = left_multiply(table_yi, mid[a])
            return carry

        lax.fori_loop(0, QC, y_inverse, 0)

        for dy, dz in near:
            ys = pl.ds(pl.multiple_of(gys[dy] * block_y, 8), block_y)
            zs = pl.ds(pl.multiple_of(gzs[dz] * block_z, 128), block_z)
            src, dst = send3.at[part, ys, zs], out.at[part, row_x]
            if dy or dz:
                send(src, dst, 6 + c, {"gy": gys[dy], "gz": gzs[dz]})
            else:
                keep(src, dst, 6 + c)

    for c in range(CHUNKS):
        received(out.at[pl.ds(c * QC, QC)], 6 + c)

    sent(2 * (group - 1) * block_y * block_z // COLS, 0)
    pltpu.make_async_copy(others, others, ssem.at[1]).wait()
    pltpu.make_async_copy(far_others, far_others, ssem.at[8]).wait()
    for c in range(CHUNKS):
        sent((devices - 1) * QC, 2 + c)
        sent((devices - 1) * QC, 4 + c)
        sent((group - 1) * QC * block_y * block_z // COLS, 6 + c)


def solution(mesh):
    sizes = tuple(mesh.shape[axis] for axis in ("gx", "gy", "gz"))
    bz = basis(NZ)
    tz = np.stack(halves(bz))
    by, bx = basis(NY), basis(NX)
    fx2 = np.broadcast_to(wave_squared(NX)[:, None], (NX, 128)).astype(np.float32)
    fz2 = np.broadcast_to(wave_squared(NZ)[None, :], (8, NZ)).astype(np.float32)
    tables = (tz, left_table(by.T), left_table(by), left_table(bx.T), left_table(bx), fx2, fz2)

    def body(density, coupling):
        vmem = pl.BlockSpec(memory_space=pltpu.VMEM)
        block = density.shape
        return pl.pallas_call(
            functools.partial(kernel, sizes),
            out_shape=jax.ShapeDtypeStruct((NQ,) + block, F32),
            in_specs=[vmem, pl.BlockSpec(memory_space=pltpu.SMEM)] + [vmem] * len(tables),
            out_specs=vmem,
            scratch_shapes=[
                pltpu.VMEM((block[0] + 4, block[1] + 16, block[2]), F32),
                pltpu.VMEM((block[2] + 16, block[0] * block[1]), F32),
                pltpu.VMEM((2, 2, block[0] * block[1]), F32),
                pltpu.VMEM((2, 2, block[0] * block[1]), F32),
                pltpu.VMEM((2, NY, NZ), F32),
                pltpu.VMEM(block, F32),
                pltpu.VMEM((2, 1, 128), F32),
                pltpu.VMEM((sizes[1] * sizes[2], 1, 128), F32),
                pltpu.VMEM((sizes[0], 1, 128), F32),
                pltpu.VMEM((NQ, NY, NZ), F32),
                pltpu.VMEM((QC, NY, NZ), F32),
                pltpu.VMEM((NQ, NY, NZ), F32),
                pltpu.VMEM((NQ, NX, COLS), F32),
                pltpu.VMEM((NQ, NX, COLS), F32),
                pltpu.VMEM((SUMS, NX, COLS), F32),
                pltpu.VMEM((QC, NX, COLS), F32),
                pltpu.VMEM((NQ, NX, COLS), F32),
                pltpu.VMEM((NQ, NY, NZ), F32),
                pltpu.VMEM((NQ, NY, NZ), F32),
                pltpu.SemaphoreType.DMA((9,)),
                pltpu.SemaphoreType.DMA((9,)),
                pltpu.SemaphoreType.DMA((8,)),
                pltpu.SemaphoreType.DMA((8,)),
            ],
            compiler_params=pltpu.CompilerParams(
                collective_id=0, has_side_effects=True, vmem_limit_bytes=56 * 1024 * 1024
            ),
            name="convolve",
        )(density, coupling, *[jnp.asarray(t) for t in tables])

    placed = (P("gx", "gy", "gz"), P())
    return jax.shard_map(
        body, mesh=mesh, in_specs=placed, out_specs=P(None, "gx", "gy", "gz"), check_vma=False
    )
```

```python
import functools
import math

import jax
import jax.numpy as jnp
import numpy as np
from jax import lax
from jax.experimental import pallas as pl
from jax.experimental.pallas import tpu as pltpu
from jax.sharding import PartitionSpec as P

MESH = pl.DeviceIdType.MESH
F32 = jnp.float32
BF16 = jnp.bfloat16

NQ = 14
NX, NY, NZ = 128, 64, 512
FORWARD = (5, 9)
BACKWARD = (4, 5, 5)
KNOTS = NQ + 2
COLS = NY * NZ // NX
SUMS = 2 * NQ - 1

ZAB = 0.8491 / 9.0
Q_CUT = 5.0
STEP = 0.07
LOCAL = 0.25
LAM = math.sqrt(3.0) - 2.0
FIRST_LINES, FIRST_BACK = 3, 3 + len(FORWARD)
FIRST_OUT = FIRST_BACK + len(BACKWARD)
SLOTS = FIRST_OUT + len(BACKWARD)
Y_SCALE = math.sqrt(2.0 / NY)


def frequencies(length):
    half = length // 2
    return np.array(list(range(half + 1)) + list(range(1, half)), dtype=np.float64)


def basis(length):
    half = length // 2
    points = np.arange(length)[:, None]
    waves = frequencies(length)[None, :]
    angle = 2.0 * np.pi / length * np.mod(points * waves, length)
    table = np.where(np.arange(length)[None, :] <= half, np.cos(angle), np.sin(angle))
    scale = np.full((1, length), math.sqrt(2.0 / length))
    scale[0, 0] = scale[0, half] = math.sqrt(1.0 / length)
    return table * scale


def spans(counts):
    starts = [sum(counts[:k]) for k in range(len(counts))]
    return list(enumerate(zip(starts, counts)))


def hops(offset):
    dx, dy, dz = offset
    along_y = (0, 1, 2, 1)[dx // 4 * 2 + dz // 2]
    return min(dy, 4 - dy) + min(dx % 4, 4 - dx % 4) + along_y


def far_first():
    offsets = [(dx, dy, dz) for dx in range(8) for dy in range(4) for dz in range(4)][1:]
    shuffled = [offsets[k] for k in np.random.RandomState(3).permutation(len(offsets))]
    return sorted(shuffled, key=lambda offset: -hops(offset))


ORDER = far_first()


def halves(table):
    high = table.astype(BF16)
    low = (table - high.astype(np.float64)).astype(BF16)
    return high, low


def left_table(table):
    high, low = halves(table)
    return np.concatenate([high, high, low], axis=1)


def wave_squared(index, length):
    wave = jnp.where(index <= length // 2, index, index - length // 2).astype(F32)
    wave = wave * (2.0 * math.pi / length)
    return wave * wave


def split(value):
    high = value.astype(BF16)
    return high, (value - high.astype(F32)).astype(BF16)


def left_multiply(table, value):
    high, low = split(value)
    return jnp.dot(table, jnp.concatenate([high, low, high], axis=0), preferred_element_type=F32)


def right_multiply(value, table_ref, transposed):
    high, low = split(value)
    rows = jnp.concatenate([high, low, high], axis=1)
    side = 1 if transposed else 0
    weights = jnp.concatenate([table_ref[0], table_ref[0], table_ref[1]], axis=side)
    return lax.dot_general(rows, weights, (((1,), (side,)), ((), ())), preferred_element_type=F32)


def kernel(
    sizes, dens, coup, tz_hbm, ty_f, ty_i, tx_f, tx_i, out,
    ext, zext, zsend, zhalo, planes, q_buf, top_src, near_tops, far_tops, thetas, mid, send1, recv1, spec, gain, prod, send2, recv2, send3,
    tz, table_sem, ssem, rsem, hsend, hrecv,
):
    devices = NX
    nx, ny, nz = sizes
    group = ny * nz
    ix, iy, iz = lax.axis_index("gx"), lax.axis_index("gy"), lax.axis_index("gz")
    me = (ix * ny + iy) * nz + iz
    block_x, block_y, block_z = NX // nx, NY // ny, NZ // nz
    per_row = NZ // COLS

    def send(src, dst, slot, to):
        pltpu.make_async_remote_copy(
            src, dst, ssem.at[slot], rsem.at[slot], device_id=to, device_id_type=MESH
        ).start()

    def keep(src, dst, slot):
        pltpu.make_async_copy(src, dst, rsem.at[slot]).start()

    def received(ref, slot):
        pltpu.make_async_copy(ref, ref, rsem.at[slot]).wait()

    def sent(rows, slot):
        full, rest = divmod(rows, NX)
        if full:
            part = recv1.at[pl.ds(0, full)]
            pltpu.make_async_copy(part, part, ssem.at[slot]).wait()
        if rest // 8:
            part = recv1.at[0, pl.ds(0, rest // 8 * 8)]
            pltpu.make_async_copy(part, part, ssem.at[slot]).wait()
        for _ in range(rest % 8):
            part = recv1.at[0, 0]
            pltpu.make_async_copy(part, part, ssem.at[slot]).wait()

    load_table = pltpu.make_async_copy(tz_hbm, tz, table_sem)
    load_table.start()
    z_len = nx // 2
    y_hi, z_at, y_lo, core = lax.div(ix, z_len), lax.rem(ix, z_len), lax.div(iz, 2), lax.rem(iz, 2)
    gys = [lax.rem(iy + j, ny) for j in range(ny)]
    gzs = [
        (1 - y_lo if j // 2 else y_lo) * 2 + (1 - core if j % 2 else core) for j in range(nz)
    ]
    gxs = [
        (1 - y_hi if j // z_len else y_hi) * z_len + lax.rem(z_at + j % z_len, z_len)
        for j in range(nx)
    ]
    near = [(dy, dz) for dz in range(nz) for dy in range(ny)]
    barrier = pltpu.get_barrier_semaphore()
    for dy, dz in near[1:]:
        pl.semaphore_signal(
            barrier, inc=1, device_id={"gy": gys[dy], "gz": gzs[dz]}, device_id_type=MESH
        )
    for dx in range(1, nx):
        pl.semaphore_signal(
            barrier, inc=1, device_id={"gx": gxs[dx]}, device_id_type=MESH
        )
    block = dens[...]
    ext[pl.ds(2, block_x), pl.ds(8, block_y), :] = block
    turned = block.reshape(block_x * block_y, block_z).T
    zext[pl.ds(8, block_z), :] = turned
    zsend[0] = turned[:2]
    zsend[1] = turned[block_z - 2 :]
    pl.semaphore_wait(barrier, group - 1 + nx - 1)

    halos = []

    def halo(src, dst, to):
        slot = len(halos)
        copy = pltpu.make_async_remote_copy(
            src, dst, hsend.at[slot], hrecv.at[slot], device_id=to, device_id_type=MESH
        )
        copy.start()
        halos.append(copy)

    low_x, high_x = {"gx": lax.rem(ix + nx - 1, nx)}, {"gx": lax.rem(ix + 1, nx)}
    low_y, high_y = {"gy": gys[ny - 1]}, {"gy": gys[1]}
    low_z, high_z = {"gz": lax.rem(iz + nz - 1, nz)}, {"gz": lax.rem(iz + 1, nz)}
    inner_x, inner_y = pl.ds(2, block_x), pl.ds(8, block_y)
    halo(dens.at[pl.ds(0, 2)], ext.at[pl.ds(block_x + 2, 2), inner_y], low_x)
    halo(dens.at[pl.ds(block_x - 2, 2)], ext.at[pl.ds(0, 2), inner_y], high_x)
    for k in range(2):
        halo(dens.at[:, k, :], ext.at[inner_x, block_y + 8 + k, :], low_y)
        halo(dens.at[:, block_y - 2 + k, :], ext.at[inner_x, 6 + k, :], high_y)
    halo(zsend.at[0], zhalo.at[1], low_z)
    halo(zsend.at[1], zhalo.at[0], high_z)

    here, row_x = iy * nz + iz, iy * nz + iz
    here_y = pl.ds(pl.multiple_of(iy * block_y, 8), block_y)
    here_z = pl.ds(pl.multiple_of(iz * block_z, 128), block_z)

    def rows_out(src, which):
        for dy, dz in near:
            row = gys[dy] * nz + gzs[dz]
            dst = planes.at[which, here_y, here_z]
            if dy or dz:
                send(src.at[row], dst, 0, {"gy": gys[dy], "gz": gzs[dz]})
            else:
                keep(src.at[row], dst, 0)

    for copy in halos:
        copy.wait()

    zext[6:8, :] = zhalo[0]
    zext[pl.ds(block_z + 8, 2), :] = zhalo[1]

    def squared_slope(at):
        slope = (8.0 * (at(1) - at(-1)) - (at(2) - at(-2))) / 12.0
        return slope * slope

    grad_sq = squared_slope(lambda o: ext[pl.ds(2 + o, block_x), inner_y, :])
    grad_sq = grad_sq + squared_slope(lambda o: ext[inner_x, pl.ds(8 + o, block_y), :])
    along_z = squared_slope(lambda o: zext[pl.ds(8 + o, block_z), :])
    grad_sq = grad_sq + along_z.T.reshape(block_x, block_y, block_z)
    cube = (3.0 * math.pi * math.pi) * block
    fermi_k = jnp.exp(jnp.log(cube) / 3.0)
    fermi_k = fermi_k - (fermi_k - cube / (fermi_k * fermi_k)) * (1.0 / 3.0)
    reduced = grad_sq / (4.0 * fermi_k * fermi_k * block * block)
    scaled = fermi_k * (1.0 + ZAB * reduced) / Q_CUT
    series = jnp.full_like(scaled, 1.0 / 12.0)
    for order in range(11, 0, -1):
        series = series * scaled + 1.0 / order
    q_zero = Q_CUT * (1.0 - jnp.exp(-(series * scaled)))
    q_buf[...] = q_zero
    top = jnp.max(jnp.max(q_zero, axis=0), axis=0, keepdims=True)
    top = jnp.broadcast_to(jnp.max(top, axis=1, keepdims=True), (1, 128))
    top_src[0] = top
    near_tops[here] = top

    for dy, dz in near[1:]:
        send(top_src.at[0], near_tops.at[here], 1, {"gy": gys[dy], "gz": gzs[dz]})
    rows_out(q_buf, 1)
    rows_out(dens, 0)
    others = near_tops.at[pl.ds(0, group - 1)]
    received(others, 1)
    top = jnp.max(near_tops[...], axis=0)
    top_src[1] = top
    far_tops[ix] = top
    for dx in range(1, nx):
        send(top_src.at[1], far_tops.at[ix], 2, {"gx": gxs[dx]})
    far_others = far_tops.at[pl.ds(0, nx - 1)]
    received(far_others, 2)
    q_top = jnp.max(far_tops[...])
    received(planes, 0)

    inv_top = 1.0 / jnp.broadcast_to(q_top, (8, 128))
    weight = math.sqrt(3.0) / 6.0

    def theta_rows(r, carry):
        rows = pl.ds(pl.multiple_of(r * 8, 8), 8)
        for lane in range(NZ // 128):
            lanes = pl.ds(lane * 128, 128)
            value = planes[0, rows, lanes] * weight
            position = jnp.maximum(
                (NQ - 1.0) + jnp.log(planes[1, rows, lanes] * inv_top) / STEP, 0.0
            )
            splines = []
            for j in range(-1, NQ + 1):
                offset = jnp.abs(position - float(j))
                wide = jnp.maximum(2.0 - offset, 0.0)
                narrow = jnp.maximum(1.0 - offset, 0.0)
                splines.append(wide * wide * wide - 4.0 * (narrow * narrow * narrow))
            up = [splines[0]]
            for j in range(1, KNOTS - 1):
                up.append(splines[j] + LAM * up[-1])
            down = splines[KNOTS - 1]
            for a in range(NQ - 1, -1, -1):
                below = LAM * down
                thetas[a, rows, lanes] = (up[a + 1] + below) * value
                down = splines[a + 1] + below
        return carry

    lax.fori_loop(0, NY // 8, theta_rows, 0)

    table_yf = ty_f[...]
    load_table.wait()
    rows_of = [lax.div(g, per_row) for g in gzs]
    cols_of = [pl.ds(pl.multiple_of(lax.rem(g, per_row) * COLS, 128), COLS) for g in gzs]

    def to_all(issue):
        for dx, dy, dz in ORDER:
            p = (gxs[dx] * ny + gys[dy]) * nz + gzs[dz]
            row = (gxs[dx] * ny + gys[dy]) * (nz // per_row) + rows_of[dz]
            issue(p, row, cols_of[dz], {"gx": gxs[dx], "gy": gys[dy], "gz": gzs[dz]})

    my_row, my_cols = lax.div(me, per_row), pl.ds(pl.multiple_of(lax.rem(me, per_row) * COLS, 128), COLS)
    for c, (first, count) in spans(FORWARD):
        part = pl.ds(first, count)

        def y_forward(a, carry, first=first):
            mid[a] = left_multiply(table_yf, thetas[first + a])
            return carry

        lax.fori_loop(0, count, y_forward, 0, unroll=True)
        rows = right_multiply(mid[pl.ds(0, count)].reshape(count * NY, NZ), tz, False)
        send1[part] = rows.reshape(count, NY, NZ)

        slot = FIRST_LINES + c
        to_all(lambda p, row, cols, to: send(send1.at[part, row, cols], recv1.at[part, me], slot, to))
        keep(send1.at[part, my_row, my_cols], recv1.at[part, me], slot)

    col = lax.broadcasted_iota(jnp.int32, (8, COLS), 1) + lax.rem(me, per_row) * COLS
    yz2 = wave_squared(my_row, NY) + wave_squared(col, NZ)
    top_sq = jnp.broadcast_to(q_top * q_top, (8, COLS))

    def gain_rows(r, carry):
        rows = pl.ds(pl.multiple_of(r * 8, 8), 8)
        k_sq = wave_squared(lax.broadcasted_iota(jnp.int32, (8, COLS), 0) + r * 8, NX) + yz2
        for s in range(SUMS):
            mass = top_sq * math.exp(-STEP * (2 * NQ - 2 - s))
            gain[s, rows, :] = LOCAL + mass / (k_sq + mass)
        return carry

    lax.fori_loop(0, NX // 8, gain_rows, 0)

    table_xf, table_xi = tx_f[...], tx_i[...]
    for c, (first, count) in spans(FORWARD):
        received(recv1.at[pl.ds(first, count)], FIRST_LINES + c)

        def x_forward(a, carry, first=first):
            spec[first + a] = left_multiply(table_xf, recv1[first + a])
            return carry

        lax.fori_loop(0, count, x_forward, 0, unroll=True)

    for c, (first, count) in spans(BACKWARD):
        part = pl.ds(first, count)

        def couple(r, carry, first=first, count=count):
            rows = pl.ds(pl.multiple_of(r * 8, 8), 8)
            for lane in range(COLS // 128):
                lanes = pl.ds(lane * 128, 128)
                source = [spec[b, rows, lanes] for b in range(NQ)]
                factor = {}
                for s in range(first, first + count + NQ - 1):
                    factor[s] = gain[s, rows, lanes]
                for a in range(count):
                    total = None
                    for b in range(NQ):
                        term = (coup[first + a, b] * factor[first + a + b]) * source[b]
                        total = term if total is None else total + term
                    prod[a, rows, lanes] = total
            return carry

        lax.fori_loop(0, NX // 8, couple, 0)

        def x_inverse(a, carry, first=first):
            send2[first + a] = left_multiply(table_xi, prod[a])
            return carry

        lax.fori_loop(0, count, x_inverse, 0, unroll=True)

        slot = FIRST_BACK + c
        to_all(lambda p, row, cols, to: send(send2.at[part, p], recv2.at[part, my_row, my_cols], slot, to))
        keep(send2.at[part, me], recv2.at[part, my_row, my_cols], slot)

    table_yi = ty_i[...]
    for c, (first, count) in spans(BACKWARD):
        part = pl.ds(first, count)
        received(recv2.at[part], FIRST_BACK + c)
        rows = right_multiply(recv2[part].reshape(count * NY, NZ), tz, True)
        mid[pl.ds(0, count)] = rows.reshape(count, NY, NZ)

        def y_inverse(a, carry, first=first):
            send3[first + a] = left_multiply(table_yi, mid[a])
            return carry

        lax.fori_loop(0, count, y_inverse, 0, unroll=True)

        for dy, dz in near:
            ys = pl.ds(pl.multiple_of(gys[dy] * block_y, 8), block_y)
            zs = pl.ds(pl.multiple_of(gzs[dz] * block_z, 128), block_z)
            src, dst = send3.at[part, ys, zs], out.at[part, row_x]
            if dy or dz:
                send(src, dst, FIRST_OUT + c, {"gy": gys[dy], "gz": gzs[dz]})
            else:
                keep(src, dst, FIRST_OUT + c)

    for c, (first, count) in spans(BACKWARD):
        received(out.at[pl.ds(first, count)], FIRST_OUT + c)

    sent(2 * (group - 1) * block_y * block_z // COLS, 0)
    pltpu.make_async_copy(others, others, ssem.at[1]).wait()
    pltpu.make_async_copy(far_others, far_others, ssem.at[2]).wait()
    for c, (_, count) in spans(FORWARD):
        sent((devices - 1) * count, FIRST_LINES + c)
    for c, (_, count) in spans(BACKWARD):
        sent((devices - 1) * count, FIRST_BACK + c)
        sent((group - 1) * count * block_y * block_z // COLS, FIRST_OUT + c)


def solution(mesh):
    sizes = tuple(mesh.shape[axis] for axis in ("gx", "gy", "gz"))
    bz = basis(NZ)
    tz = np.stack(halves(bz))
    by, bx = basis(NY), basis(NX)
    tables = (tz, left_table(by.T), left_table(by / Y_SCALE), left_table(bx.T), left_table(bx))

    def body(density, coupling):
        vmem, anywhere = (pl.BlockSpec(memory_space=space) for space in (pltpu.VMEM, pl.ANY))
        block = density.shape
        fields = pl.pallas_call(
            functools.partial(kernel, sizes),
            out_shape=jax.ShapeDtypeStruct((NQ,) + block, F32),
            in_specs=[vmem, pl.BlockSpec(memory_space=pltpu.SMEM), anywhere] + [vmem] * (len(tables) - 1),
            out_specs=anywhere,
            scratch_shapes=[
                pltpu.VMEM((block[0] + 4, block[1] + 16, block[2]), F32),
                pltpu.VMEM((block[2] + 16, block[0] * block[1]), F32),
                pltpu.VMEM((2, 2, block[0] * block[1]), F32),
                pltpu.VMEM((2, 2, block[0] * block[1]), F32),
                pltpu.VMEM((2, NY, NZ), F32),
                pltpu.VMEM(block, F32),
                pltpu.VMEM((2, 1, 128), F32),
                pltpu.VMEM((sizes[1] * sizes[2], 1, 128), F32),
                pltpu.VMEM((sizes[0], 1, 128), F32),
                pltpu.VMEM((NQ, NY, NZ), F32),
                pltpu.VMEM((max(FORWARD + BACKWARD), NY, NZ), F32),
                pltpu.VMEM((NQ, NY, NZ), F32),
                pltpu.VMEM((NQ, NX, COLS), F32),
                pltpu.VMEM((NQ, NX, COLS), F32),
                pltpu.VMEM((SUMS, NX, COLS), F32),
                pltpu.VMEM((max(BACKWARD), NX, COLS), F32),
                pltpu.VMEM((NQ, NX, COLS), F32),
                pltpu.VMEM((NQ, NY, NZ), F32),
                pltpu.VMEM((NQ, NY, NZ), F32),
                pltpu.VMEM((2, NZ, NZ), BF16),
                pltpu.SemaphoreType.DMA,
                pltpu.SemaphoreType.DMA((SLOTS,)),
                pltpu.SemaphoreType.DMA((SLOTS,)),
                pltpu.SemaphoreType.DMA((8,)),
                pltpu.SemaphoreType.DMA((8,)),
            ],
            compiler_params=pltpu.CompilerParams(
                collective_id=0, has_side_effects=True, vmem_limit_bytes=56 * 1024 * 1024
            ),
            name="convolve",
        )(density, coupling, *[jnp.asarray(t) for t in tables])
        return fields * Y_SCALE

    placed = (P("gx", "gy", "gz"), P())
    return jax.shard_map(
        body, mesh=mesh, in_specs=placed, out_specs=P(None, "gx", "gy", "gz"), check_vma=False
    )
```

```python
import functools
import math

import jax
import jax.numpy as jnp
import numpy as np
from jax import lax
from jax.experimental import pallas as pl
from jax.experimental.pallas import tpu as pltpu
from jax.sharding import PartitionSpec as P

MESH = pl.DeviceIdType.MESH
F32 = jnp.float32
BF16 = jnp.bfloat16

NQ = 14
NX, NY, NZ = 128, 64, 512
FORWARD = (5, 9)
BACKWARD = (4, 5, 5)
KNOTS = NQ + 2
COLS = NY * NZ // NX
SUMS = 2 * NQ - 1

ZAB = 0.8491 / 9.0
Q_CUT = 5.0
STEP = 0.07
LOCAL = 0.25
LAM = math.sqrt(3.0) - 2.0
FIRST_LINES, FIRST_BACK = 3, 3 + len(FORWARD)
FIRST_OUT = FIRST_BACK + len(BACKWARD)
SLOTS = FIRST_OUT + len(BACKWARD)


def frequencies(length):
    half = length // 2
    return np.array(list(range(half + 1)) + list(range(1, half)), dtype=np.float64)


def basis(length):
    half = length // 2
    points = np.arange(length)[:, None]
    waves = frequencies(length)[None, :]
    angle = 2.0 * np.pi / length * np.mod(points * waves, length)
    table = np.where(np.arange(length)[None, :] <= half, np.cos(angle), np.sin(angle))
    scale = np.full((1, length), math.sqrt(2.0 / length))
    scale[0, 0] = scale[0, half] = math.sqrt(1.0 / length)
    return table * scale


def spans(counts):
    starts = [sum(counts[:k]) for k in range(len(counts))]
    return list(enumerate(zip(starts, counts)))


def hops(offset):
    dx, dy, dz = offset
    along_y = (0, 1, 2, 1)[dx // 4 * 2 + dz // 2]
    return min(dy, 4 - dy) + min(dx % 4, 4 - dx % 4) + along_y


def far_first():
    offsets = [(dx, dy, dz) for dx in range(8) for dy in range(4) for dz in range(4)][1:]
    shuffled = [offsets[k] for k in np.random.RandomState(3).permutation(len(offsets))]
    return sorted(shuffled, key=lambda offset: -hops(offset))


ORDER = far_first()


def halves(table):
    high = table.astype(BF16)
    low = (table - high.astype(np.float64)).astype(BF16)
    return high, low


def left_table(table):
    high, low = halves(table)
    return np.concatenate([high, high, low], axis=1)


def wave_squared(index, length):
    wave = jnp.where(index <= length // 2, index, index - length // 2).astype(F32)
    wave = wave * (2.0 * math.pi / length)
    return wave * wave


def split(value):
    high = value.astype(BF16)
    return high, (value - high.astype(F32)).astype(BF16)


def left_multiply(table, value):
    high, low = split(value)
    return jnp.dot(table, jnp.concatenate([high, low, high], axis=0), preferred_element_type=F32)


def right_multiply(value, table_ref, transposed):
    high, low = split(value)
    rows = jnp.concatenate([high, low, high], axis=1)
    side = 1 if transposed else 0
    weights = jnp.concatenate([table_ref[0], table_ref[0], table_ref[1]], axis=side)
    return lax.dot_general(rows, weights, (((1,), (side,)), ((), ())), preferred_element_type=F32)


def kernel(
    sizes, dens_in, coup_in, tz_in, ty_f_in, ty_i_in, tx_f_in, tx_i_in, out,
    ext, zext, zsend, zhalo, planes, q_buf, top_src, near_tops, far_tops, thetas, mid, send1, recv1, spec, gain, prod, send2, recv2, send3,
    dens, coup, tz, ty_f, ty_i, tx_f, tx_i, load_sem, ssem, rsem, hsend, hrecv,
):
    devices = NX
    nx, ny, nz = sizes
    group = ny * nz
    ix, iy, iz = lax.axis_index("gx"), lax.axis_index("gy"), lax.axis_index("gz")
    me = (ix * ny + iy) * nz + iz
    block_x, block_y, block_z = NX // nx, NY // ny, NZ // nz
    per_row = NZ // COLS

    def send(src, dst, slot, to):
        pltpu.make_async_remote_copy(
            src, dst, ssem.at[slot], rsem.at[slot], device_id=to, device_id_type=MESH
        ).start()

    def keep(src, dst, slot):
        pltpu.make_async_copy(src, dst, rsem.at[slot]).start()

    def received(ref, slot):
        pltpu.make_async_copy(ref, ref, rsem.at[slot]).wait()

    def sent(rows, slot):
        full, rest = divmod(rows, NX)
        if full:
            part = recv1.at[pl.ds(0, full)]
            pltpu.make_async_copy(part, part, ssem.at[slot]).wait()
        if rest // 8:
            part = recv1.at[0, pl.ds(0, rest // 8 * 8)]
            pltpu.make_async_copy(part, part, ssem.at[slot]).wait()
        for _ in range(rest % 8):
            part = recv1.at[0, 0]
            pltpu.make_async_copy(part, part, ssem.at[slot]).wait()

    inputs = ((dens_in, dens), (coup_in, coup), (tz_in, tz), (ty_f_in, ty_f), (ty_i_in, ty_i))
    inputs = inputs + ((tx_f_in, tx_f), (tx_i_in, tx_i))
    loads = [pltpu.make_async_copy(a, b, load_sem.at[k]) for k, (a, b) in enumerate(inputs)]
    for load in loads:
        load.start()
    z_len = nx // 2
    y_hi, z_at, y_lo, core = lax.div(ix, z_len), lax.rem(ix, z_len), lax.div(iz, 2), lax.rem(iz, 2)
    gys = [lax.rem(iy + j, ny) for j in range(ny)]
    gzs = [
        (1 - y_lo if j // 2 else y_lo) * 2 + (1 - core if j % 2 else core) for j in range(nz)
    ]
    gxs = [
        (1 - y_hi if j // z_len else y_hi) * z_len + lax.rem(z_at + j % z_len, z_len)
        for j in range(nx)
    ]
    near = [(dy, dz) for dz in range(nz) for dy in range(ny)]
    barrier = pltpu.get_barrier_semaphore()
    for dy, dz in near[1:]:
        pl.semaphore_signal(
            barrier, inc=1, device_id={"gy": gys[dy], "gz": gzs[dz]}, device_id_type=MESH
        )
    for dx in range(1, nx):
        pl.semaphore_signal(
            barrier, inc=1, device_id={"gx": gxs[dx]}, device_id_type=MESH
        )
    loads[0].wait()
    block = dens[...]
    ext[pl.ds(2, block_x), pl.ds(8, block_y), :] = block
    turned = block.reshape(block_x * block_y, block_z).T
    zext[pl.ds(8, block_z), :] = turned
    zsend[0] = turned[:2]
    zsend[1] = turned[block_z - 2 :]
    pl.semaphore_wait(barrier, group - 1 + nx - 1)

    halos = []

    def halo(src, dst, to):
        slot = len(halos)
        copy = pltpu.make_async_remote_copy(
            src, dst, hsend.at[slot], hrecv.at[slot], device_id=to, device_id_type=MESH
        )
        copy.start()
        halos.append(copy)

    low_x, high_x = {"gx": lax.rem(ix + nx - 1, nx)}, {"gx": lax.rem(ix + 1, nx)}
    low_y, high_y = {"gy": gys[ny - 1]}, {"gy": gys[1]}
    low_z, high_z = {"gz": lax.rem(iz + nz - 1, nz)}, {"gz": lax.rem(iz + 1, nz)}
    inner_x, inner_y = pl.ds(2, block_x), pl.ds(8, block_y)
    halo(dens.at[pl.ds(0, 2)], ext.at[pl.ds(block_x + 2, 2), inner_y], low_x)
    halo(dens.at[pl.ds(block_x - 2, 2)], ext.at[pl.ds(0, 2), inner_y], high_x)
    for k in range(2):
        halo(dens.at[:, k, :], ext.at[inner_x, block_y + 8 + k, :], low_y)
        halo(dens.at[:, block_y - 2 + k, :], ext.at[inner_x, 6 + k, :], high_y)
    halo(zsend.at[0], zhalo.at[1], low_z)
    halo(zsend.at[1], zhalo.at[0], high_z)

    here, row_x = iy * nz + iz, iy * nz + iz
    here_y = pl.ds(pl.multiple_of(iy * block_y, 8), block_y)
    here_z = pl.ds(pl.multiple_of(iz * block_z, 128), block_z)

    def rows_out(src, which):
        for dy, dz in near:
            row = gys[dy] * nz + gzs[dz]
            dst = planes.at[which, here_y, here_z]
            if dy or dz:
                send(src.at[row], dst, 0, {"gy": gys[dy], "gz": gzs[dz]})
            else:
                keep(src.at[row], dst, 0)

    for copy in halos:
        copy.wait()

    zext[6:8, :] = zhalo[0]
    zext[pl.ds(block_z + 8, 2), :] = zhalo[1]

    def squared_slope(at):
        slope = (8.0 * (at(1) - at(-1)) - (at(2) - at(-2))) / 12.0
        return slope * slope

    grad_sq = squared_slope(lambda o: ext[pl.ds(2 + o, block_x), inner_y, :])
    grad_sq = grad_sq + squared_slope(lambda o: ext[inner_x, pl.ds(8 + o, block_y), :])
    along_z = squared_slope(lambda o: zext[pl.ds(8 + o, block_z), :])
    grad_sq = grad_sq + along_z.T.reshape(block_x, block_y, block_z)
    cube = (3.0 * math.pi * math.pi) * block
    fermi_k = jnp.exp(jnp.log(cube) / 3.0)
    fermi_k = fermi_k - (fermi_k - cube / (fermi_k * fermi_k)) * (1.0 / 3.0)
    reduced = grad_sq / (4.0 * fermi_k * fermi_k * block * block)
    scaled = fermi_k * (1.0 + ZAB * reduced) / Q_CUT
    series = jnp.full_like(scaled, 1.0 / 12.0)
    for order in range(11, 0, -1):
        series = series * scaled + 1.0 / order
    q_zero = Q_CUT * (1.0 - jnp.exp(-(series * scaled)))
    q_buf[...] = q_zero
    top = jnp.max(jnp.max(q_zero, axis=0), axis=0, keepdims=True)
    top = jnp.broadcast_to(jnp.max(top, axis=1, keepdims=True), (1, 128))
    top_src[0] = top
    near_tops[here] = top

    for dy, dz in near[1:]:
        send(top_src.at[0], near_tops.at[here], 1, {"gy": gys[dy], "gz": gzs[dz]})
    rows_out(q_buf, 1)
    rows_out(dens, 0)
    others = near_tops.at[pl.ds(0, group - 1)]
    received(others, 1)
    top = jnp.max(near_tops[...], axis=0)
    top_src[1] = top
    far_tops[ix] = top
    for dx in range(1, nx):
        send(top_src.at[1], far_tops.at[ix], 2, {"gx": gxs[dx]})
    far_others = far_tops.at[pl.ds(0, nx - 1)]
    received(far_others, 2)
    q_top = jnp.max(far_tops[...])
    received(planes, 0)

    inv_top = 1.0 / jnp.broadcast_to(q_top, (8, 128))
    weight = math.sqrt(3.0) / 6.0

    def theta_rows(r, carry):
        rows = pl.ds(pl.multiple_of(r * 8, 8), 8)
        for lane in range(NZ // 128):
            lanes = pl.ds(lane * 128, 128)
            value = planes[0, rows, lanes] * weight
            position = jnp.maximum(
                (NQ - 1.0) + jnp.log(planes[1, rows, lanes] * inv_top) / STEP, 0.0
            )
            splines = []
            for j in range(-1, NQ + 1):
                offset = jnp.abs(position - float(j))
                wide = jnp.maximum(2.0 - offset, 0.0)
                narrow = jnp.maximum(1.0 - offset, 0.0)
                splines.append(wide * wide * wide - 4.0 * (narrow * narrow * narrow))
            up = [splines[0]]
            for j in range(1, KNOTS - 1):
                up.append(splines[j] + LAM * up[-1])
            down = splines[KNOTS - 1]
            for a in range(NQ - 1, -1, -1):
                below = LAM * down
                thetas[a, rows, lanes] = (up[a + 1] + below) * value
                down = splines[a + 1] + below
        return carry

    lax.fori_loop(0, NY // 8, theta_rows, 0)

    for load in loads[1:]:
        load.wait()
    table_yf = ty_f[...]
    rows_of = [lax.div(g, per_row) for g in gzs]
    cols_of = [pl.ds(pl.multiple_of(lax.rem(g, per_row) * COLS, 128), COLS) for g in gzs]

    def to_all(issue):
        for dx, dy, dz in ORDER:
            p = (gxs[dx] * ny + gys[dy]) * nz + gzs[dz]
            row = (gxs[dx] * ny + gys[dy]) * (nz // per_row) + rows_of[dz]
            issue(p, row, cols_of[dz], {"gx": gxs[dx], "gy": gys[dy], "gz": gzs[dz]})

    my_row, my_cols = lax.div(me, per_row), pl.ds(pl.multiple_of(lax.rem(me, per_row) * COLS, 128), COLS)
    for c, (first, count) in spans(FORWARD):
        part = pl.ds(first, count)

        def y_forward(a, carry, first=first):
            mid[a] = left_multiply(table_yf, thetas[first + a])
            return carry

        lax.fori_loop(0, count, y_forward, 0, unroll=True)
        rows = right_multiply(mid[pl.ds(0, count)].reshape(count * NY, NZ), tz, False)
        send1[part] = rows.reshape(count, NY, NZ)

        slot = FIRST_LINES + c
        to_all(lambda p, row, cols, to: send(send1.at[part, row, cols], recv1.at[part, me], slot, to))
        keep(send1.at[part, my_row, my_cols], recv1.at[part, me], slot)

    col = lax.broadcasted_iota(jnp.int32, (8, COLS), 1) + lax.rem(me, per_row) * COLS
    yz2 = wave_squared(my_row, NY) + wave_squared(col, NZ)
    top_sq = jnp.broadcast_to(q_top * q_top, (8, COLS))

    def gain_rows(r, carry):
        rows = pl.ds(pl.multiple_of(r * 8, 8), 8)
        k_sq = wave_squared(lax.broadcasted_iota(jnp.int32, (8, COLS), 0) + r * 8, NX) + yz2
        for s in range(SUMS):
            mass = top_sq * math.exp(-STEP * (2 * NQ - 2 - s))
            gain[s, rows, :] = LOCAL + mass / (k_sq + mass)
        return carry

    lax.fori_loop(0, NX // 8, gain_rows, 0)

    table_xf, table_xi = tx_f[...], tx_i[...]
    for c, (first, count) in spans(FORWARD):
        received(recv1.at[pl.ds(first, count)], FIRST_LINES + c)

        def x_forward(a, carry, first=first):
            spec[first + a] = left_multiply(table_xf, recv1[first + a])
            return carry

        lax.fori_loop(0, count, x_forward, 0, unroll=True)

    for c, (first, count) in spans(BACKWARD):
        part = pl.ds(first, count)

        def couple(r, carry, first=first, count=count):
            rows = pl.ds(pl.multiple_of(r * 8, 8), 8)
            for lane in range(COLS // 128):
                lanes = pl.ds(lane * 128, 128)
                source = [spec[b, rows, lanes] for b in range(NQ)]
                factor = {}
                for s in range(first, first + count + NQ - 1):
                    factor[s] = gain[s, rows, lanes]
                for a in range(count):
                    total = None
                    for b in range(NQ):
                        term = (coup[first + a, b] * factor[first + a + b]) * source[b]
                        total = term if total is None else total + term
                    prod[a, rows, lanes] = total
            return carry

        lax.fori_loop(0, NX // 8, couple, 0)

        def x_inverse(a, carry, first=first):
            send2[first + a] = left_multiply(table_xi, prod[a])
            return carry

        lax.fori_loop(0, count, x_inverse, 0, unroll=True)

        slot = FIRST_BACK + c
        to_all(lambda p, row, cols, to: send(send2.at[part, p], recv2.at[part, my_row, my_cols], slot, to))
        keep(send2.at[part, me], recv2.at[part, my_row, my_cols], slot)

    table_yi = ty_i[...]
    for c, (first, count) in spans(BACKWARD):
        part = pl.ds(first, count)
        received(recv2.at[part], FIRST_BACK + c)
        rows = right_multiply(recv2[part].reshape(count * NY, NZ), tz, True)
        mid[pl.ds(0, count)] = rows.reshape(count, NY, NZ)

        def y_inverse(a, carry, first=first):
            send3[first + a] = left_multiply(table_yi, mid[a])
            return carry

        lax.fori_loop(0, count, y_inverse, 0, unroll=True)

        for dy, dz in near:
            ys = pl.ds(pl.multiple_of(gys[dy] * block_y, 8), block_y)
            zs = pl.ds(pl.multiple_of(gzs[dz] * block_z, 128), block_z)
            src, dst = send3.at[part, ys, zs], out.at[part, row_x]
            if dy or dz:
                send(src, dst, FIRST_OUT + c, {"gy": gys[dy], "gz": gzs[dz]})
            else:
                keep(src, dst, FIRST_OUT + c)

    for c, (first, count) in spans(BACKWARD):
        received(out.at[pl.ds(first, count)], FIRST_OUT + c)

    sent(2 * (group - 1) * block_y * block_z // COLS, 0)
    pltpu.make_async_copy(others, others, ssem.at[1]).wait()
    pltpu.make_async_copy(far_others, far_others, ssem.at[2]).wait()
    for c, (_, count) in spans(FORWARD):
        sent((devices - 1) * count, FIRST_LINES + c)
    for c, (_, count) in spans(BACKWARD):
        sent((devices - 1) * count, FIRST_BACK + c)
        sent((group - 1) * count * block_y * block_z // COLS, FIRST_OUT + c)


def write_out(fields, out, sem):
    copies = [pltpu.make_async_copy(fields.at[a], out.at[a], sem.at[a]) for a in range(NQ)]
    for copy in copies:
        copy.start()
    for copy in copies:
        copy.wait()


def solution(mesh):
    sizes = tuple(mesh.shape[axis] for axis in ("gx", "gy", "gz"))
    bz = basis(NZ)
    tz = np.stack(halves(bz))
    by, bx = basis(NY), basis(NX)
    tables = (tz, left_table(by.T), left_table(by), left_table(bx.T), left_table(bx))

    def body(density, coupling):
        vmem, hbm = (pl.BlockSpec(memory_space=space) for space in (pltpu.VMEM, pltpu.HBM))
        block = density.shape
        fields = pl.pallas_call(
            functools.partial(kernel, sizes),
            out_shape=jax.ShapeDtypeStruct((NQ,) + block, F32),
            in_specs=[hbm] * (2 + len(tables)),
            out_specs=vmem,
            scratch_shapes=[
                pltpu.VMEM((block[0] + 4, block[1] + 16, block[2]), F32),
                pltpu.VMEM((block[2] + 16, block[0] * block[1]), F32),
                pltpu.VMEM((2, 2, block[0] * block[1]), F32),
                pltpu.VMEM((2, 2, block[0] * block[1]), F32),
                pltpu.VMEM((2, NY, NZ), F32),
                pltpu.VMEM(block, F32),
                pltpu.VMEM((2, 1, 128), F32),
                pltpu.VMEM((sizes[1] * sizes[2], 1, 128), F32),
                pltpu.VMEM((sizes[0], 1, 128), F32),
                pltpu.VMEM((NQ, NY, NZ), F32),
                pltpu.VMEM((max(FORWARD + BACKWARD), NY, NZ), F32),
                pltpu.VMEM((NQ, NY, NZ), F32),
                pltpu.VMEM((NQ, NX, COLS), F32),
                pltpu.VMEM((NQ, NX, COLS), F32),
                pltpu.VMEM((SUMS, NX, COLS), F32),
                pltpu.VMEM((max(BACKWARD), NX, COLS), F32),
                pltpu.VMEM((NQ, NX, COLS), F32),
                pltpu.VMEM((NQ, NY, NZ), F32),
                pltpu.VMEM((NQ, NY, NZ), F32),
                pltpu.VMEM(block, F32),
                pltpu.SMEM((NQ, NQ), F32),
                *[pltpu.VMEM(table.shape, BF16) for table in tables],
                pltpu.SemaphoreType.DMA((2 + len(tables),)),
                pltpu.SemaphoreType.DMA((SLOTS,)),
                pltpu.SemaphoreType.DMA((SLOTS,)),
                pltpu.SemaphoreType.DMA((8,)),
                pltpu.SemaphoreType.DMA((8,)),
            ],
            compiler_params=pltpu.CompilerParams(
                collective_id=0, has_side_effects=True, vmem_limit_bytes=40 * 1024 * 1024
            ),
            name="convolve",
        )(*[pltpu.with_memory_space_constraint(x, pltpu.HBM) for x in (density, coupling, *map(jnp.asarray, tables))])
        return pl.pallas_call(
            write_out,
            out_shape=jax.ShapeDtypeStruct((NQ,) + block, F32),
            in_specs=[vmem],
            out_specs=hbm,
            scratch_shapes=[pltpu.SemaphoreType.DMA((NQ,))],
            compiler_params=pltpu.CompilerParams(vmem_limit_bytes=4 * 1024 * 1024),
            cost_estimate=pl.CostEstimate(flops=0, bytes_accessed=8 * NQ * density.size, transcendentals=0),
            name="write_out",
        )(fields)

    placed = (P("gx", "gy", "gz"), P())
    return jax.shard_map(
        body, mesh=mesh, in_specs=placed, out_specs=P(None, "gx", "gy", "gz"), check_vma=False
    )
```

```python
import functools
import math

import jax
import jax.numpy as jnp
import numpy as np
from jax import lax
from jax.experimental import pallas as pl
from jax.experimental.pallas import tpu as pltpu
from jax.sharding import PartitionSpec as P

MESH = pl.DeviceIdType.MESH
F32 = jnp.float32
BF16 = jnp.bfloat16

NQ = 14
NX, NY, NZ = 128, 64, 512
FORWARD = (5, 9)
BACKWARD = (4, 3, 3, 4)
ROUTES = "QPQP"
KNOTS = NQ + 2
COLS = NY * NZ // NX
SUMS = 2 * NQ - 1

ZAB = 0.8491 / 9.0
Q_CUT = 5.0
STEP = 0.07
LOCAL = 0.25
LAM = math.sqrt(3.0) - 2.0
FIRST_LINES, FIRST_BACK = 3, 3 + len(FORWARD)
SLOTS = FIRST_BACK + 3 * len(BACKWARD)


def frequencies(length):
    half = length // 2
    return np.array(list(range(half + 1)) + list(range(1, half)), dtype=np.float64)


def basis(length):
    half = length // 2
    points = np.arange(length)[:, None]
    waves = frequencies(length)[None, :]
    angle = 2.0 * np.pi / length * np.mod(points * waves, length)
    table = np.where(np.arange(length)[None, :] <= half, np.cos(angle), np.sin(angle))
    scale = np.full((1, length), math.sqrt(2.0 / length))
    scale[0, 0] = scale[0, half] = math.sqrt(1.0 / length)
    return table * scale


def spans(counts):
    starts = [sum(counts[:k]) for k in range(len(counts))]
    return list(enumerate(zip(starts, counts)))


def hops(offset):
    dx, dy, dz = offset
    along_y = (0, 1, 2, 1)[dx // 4 * 2 + dz // 2]
    return min(dy, 4 - dy) + min(dx % 4, 4 - dx % 4) + along_y


def far_first():
    offsets = [(dx, dy, dz) for dx in range(8) for dy in range(4) for dz in range(4)][1:]
    shuffled = [offsets[k] for k in np.random.RandomState(3).permutation(len(offsets))]
    return sorted(shuffled, key=lambda offset: -hops(offset))


ORDER = far_first()
LINE_ORDER = [(dx, dz) for dx, dy, dz in ORDER if dy == 0] + [(0, 0)]


def halves(table):
    high = table.astype(BF16)
    low = (table - high.astype(np.float64)).astype(BF16)
    return high, low


def left_table(table):
    high, low = halves(table)
    return np.concatenate([high, high, low], axis=1)


def wave_squared(index, length):
    wave = jnp.where(index <= length // 2, index, index - length // 2).astype(F32)
    wave = wave * (2.0 * math.pi / length)
    return wave * wave


def split(value):
    high = value.astype(BF16)
    return high, (value - high.astype(F32)).astype(BF16)


def left_multiply(table, value):
    high, low = split(value)
    return jnp.dot(table, jnp.concatenate([high, low, high], axis=0), preferred_element_type=F32)


def right_multiply(value, table_ref, transposed):
    high, low = split(value)
    rows = jnp.concatenate([high, low, high], axis=1)
    side = 1 if transposed else 0
    weights = jnp.concatenate([table_ref[0], table_ref[0], table_ref[1]], axis=side)
    return lax.dot_general(rows, weights, (((1,), (side,)), ((), ())), preferred_element_type=F32)


def kernel(
    sizes, dens_in, coup_in, tz_in, ty_f_in, ty_i_in, tx_f_in, tx_i_in, out,
    ext, zext, zsend, zhalo, planes, q_buf, top_src, near_tops, far_tops, thetas, mid, send1, recv1, spec, gain, prod, send2, y_in, y_out, z_in_p, z_in_q, z_out_p, z_out_q,
    dens, coup, tz, ty_f, ty_i, tx_f, tx_i, load_sem, ssem, rsem, hsend, hrecv,
):
    devices = NX
    nx, ny, nz = sizes
    group = ny * nz
    ix, iy, iz = lax.axis_index("gx"), lax.axis_index("gy"), lax.axis_index("gz")
    me = (ix * ny + iy) * nz + iz
    block_x, block_y, block_z = NX // nx, NY // ny, NZ // nz

    def send(src, dst, slot, to):
        pltpu.make_async_remote_copy(
            src, dst, ssem.at[slot], rsem.at[slot], device_id=to, device_id_type=MESH
        ).start()

    def keep(src, dst, slot):
        pltpu.make_async_copy(src, dst, rsem.at[slot]).start()

    def received(ref, slot):
        pltpu.make_async_copy(ref, ref, rsem.at[slot]).wait()

    def sent(rows, slot):
        full, rest = divmod(rows, NX)
        if full:
            part = spec.at[pl.ds(0, full)]
            pltpu.make_async_copy(part, part, ssem.at[slot]).wait()
        if rest // 8:
            part = spec.at[0, pl.ds(0, rest // 8 * 8)]
            pltpu.make_async_copy(part, part, ssem.at[slot]).wait()
        for _ in range(rest % 8):
            part = spec.at[0, 0]
            pltpu.make_async_copy(part, part, ssem.at[slot]).wait()

    inputs = ((dens_in, dens), (coup_in, coup), (tz_in, tz), (ty_f_in, ty_f), (ty_i_in, ty_i))
    inputs = inputs + ((tx_f_in, tx_f), (tx_i_in, tx_i))
    loads = [pltpu.make_async_copy(a, b, load_sem.at[k]) for k, (a, b) in enumerate(inputs)]
    for load in loads:
        load.start()
    z_len = nx // 2
    y_hi, z_at, y_lo, core = lax.div(ix, z_len), lax.rem(ix, z_len), lax.div(iz, 2), lax.rem(iz, 2)
    gys = [lax.rem(iy + j, ny) for j in range(ny)]
    gzs = [
        (1 - y_lo if j // 2 else y_lo) * 2 + (1 - core if j % 2 else core) for j in range(nz)
    ]
    gxs = [
        (1 - y_hi if j // z_len else y_hi) * z_len + lax.rem(z_at + j % z_len, z_len)
        for j in range(nx)
    ]
    near = [(dy, dz) for dz in range(nz) for dy in range(ny)]
    barrier = pltpu.get_barrier_semaphore()
    for dy, dz in near[1:]:
        pl.semaphore_signal(
            barrier, inc=1, device_id={"gy": gys[dy], "gz": gzs[dz]}, device_id_type=MESH
        )
    for dx in range(1, nx):
        pl.semaphore_signal(
            barrier, inc=1, device_id={"gx": gxs[dx]}, device_id_type=MESH
        )
    loads[0].wait()
    block = dens[...]
    ext[pl.ds(2, block_x), pl.ds(8, block_y), :] = block
    turned = block.reshape(block_x * block_y, block_z).T
    zext[pl.ds(8, block_z), :] = turned
    zsend[0] = turned[:2]
    zsend[1] = turned[block_z - 2 :]
    pl.semaphore_wait(barrier, group - 1 + nx - 1)

    halos = []

    def halo(src, dst, to):
        slot = len(halos)
        copy = pltpu.make_async_remote_copy(
            src, dst, hsend.at[slot], hrecv.at[slot], device_id=to, device_id_type=MESH
        )
        copy.start()
        halos.append(copy)

    low_x, high_x = {"gx": lax.rem(ix + nx - 1, nx)}, {"gx": lax.rem(ix + 1, nx)}
    low_y, high_y = {"gy": gys[ny - 1]}, {"gy": gys[1]}
    low_z, high_z = {"gz": lax.rem(iz + nz - 1, nz)}, {"gz": lax.rem(iz + 1, nz)}
    inner_x, inner_y = pl.ds(2, block_x), pl.ds(8, block_y)
    halo(dens.at[pl.ds(0, 2)], ext.at[pl.ds(block_x + 2, 2), inner_y], low_x)
    halo(dens.at[pl.ds(block_x - 2, 2)], ext.at[pl.ds(0, 2), inner_y], high_x)
    for k in range(2):
        halo(dens.at[:, k, :], ext.at[inner_x, block_y + 8 + k, :], low_y)
        halo(dens.at[:, block_y - 2 + k, :], ext.at[inner_x, 6 + k, :], high_y)
    halo(zsend.at[0], zhalo.at[1], low_z)
    halo(zsend.at[1], zhalo.at[0], high_z)

    here, row_x = iy * nz + iz, iy * nz + iz
    here_y = pl.ds(pl.multiple_of(iy * block_y, 8), block_y)
    here_z = pl.ds(pl.multiple_of(iz * block_z, 128), block_z)

    def rows_out(src, which):
        for dy, dz in near:
            row = gys[dy] * nz + gzs[dz]
            dst = planes.at[which, here_y, here_z]
            if dy or dz:
                send(src.at[row], dst, 0, {"gy": gys[dy], "gz": gzs[dz]})
            else:
                keep(src.at[row], dst, 0)

    for copy in halos:
        copy.wait()

    zext[6:8, :] = zhalo[0]
    zext[pl.ds(block_z + 8, 2), :] = zhalo[1]

    def squared_slope(at):
        slope = (8.0 * (at(1) - at(-1)) - (at(2) - at(-2))) / 12.0
        return slope * slope

    grad_sq = squared_slope(lambda o: ext[pl.ds(2 + o, block_x), inner_y, :])
    grad_sq = grad_sq + squared_slope(lambda o: ext[inner_x, pl.ds(8 + o, block_y), :])
    along_z = squared_slope(lambda o: zext[pl.ds(8 + o, block_z), :])
    grad_sq = grad_sq + along_z.T.reshape(block_x, block_y, block_z)
    cube = (3.0 * math.pi * math.pi) * block
    fermi_k = jnp.exp(jnp.log(cube) / 3.0)
    fermi_k = fermi_k - (fermi_k - cube / (fermi_k * fermi_k)) * (1.0 / 3.0)
    reduced = grad_sq / (4.0 * fermi_k * fermi_k * block * block)
    scaled = fermi_k * (1.0 + ZAB * reduced) / Q_CUT
    series = jnp.full_like(scaled, 1.0 / 12.0)
    for order in range(11, 0, -1):
        series = series * scaled + 1.0 / order
    q_zero = Q_CUT * (1.0 - jnp.exp(-(series * scaled)))
    q_buf[...] = q_zero
    top = jnp.max(jnp.max(q_zero, axis=0), axis=0, keepdims=True)
    top = jnp.broadcast_to(jnp.max(top, axis=1, keepdims=True), (1, 128))
    top_src[0] = top
    near_tops[here] = top

    for dy, dz in near[1:]:
        send(top_src.at[0], near_tops.at[here], 1, {"gy": gys[dy], "gz": gzs[dz]})
    rows_out(q_buf, 1)
    rows_out(dens, 0)
    others = near_tops.at[pl.ds(0, group - 1)]
    received(others, 1)
    top = jnp.max(near_tops[...], axis=0)
    top_src[1] = top
    far_tops[ix] = top
    for dx in range(1, nx):
        send(top_src.at[1], far_tops.at[ix], 2, {"gx": gxs[dx]})
    far_others = far_tops.at[pl.ds(0, nx - 1)]
    received(far_others, 2)
    q_top = jnp.max(far_tops[...])
    received(planes, 0)

    inv_top = 1.0 / jnp.broadcast_to(q_top, (8, 128))
    weight = math.sqrt(3.0) / 6.0

    def theta_rows(r, carry):
        rows = pl.ds(pl.multiple_of(r * 8, 8), 8)
        for lane in range(NZ // 128):
            lanes = pl.ds(lane * 128, 128)
            value = planes[0, rows, lanes] * weight
            position = jnp.maximum(
                (NQ - 1.0) + jnp.log(planes[1, rows, lanes] * inv_top) / STEP, 0.0
            )
            splines = []
            for j in range(-1, NQ + 1):
                offset = jnp.abs(position - float(j))
                wide = jnp.maximum(2.0 - offset, 0.0)
                narrow = jnp.maximum(1.0 - offset, 0.0)
                splines.append(wide * wide * wide - 4.0 * (narrow * narrow * narrow))
            up = [splines[0]]
            for j in range(1, KNOTS - 1):
                up.append(splines[j] + LAM * up[-1])
            down = splines[KNOTS - 1]
            for a in range(NQ - 1, -1, -1):
                below = LAM * down
                thetas[a, rows, lanes] = (up[a + 1] + below) * value
                down = splines[a + 1] + below
        return carry

    lax.fori_loop(0, NY // 8, theta_rows, 0)

    for load in loads[1:]:
        load.wait()
    table_yf = ty_f[...]
    quarter = [pl.ds(pl.multiple_of(g * 128, 128), 128) for g in gys]
    z_part = [pl.ds(pl.multiple_of(g * block_z, 128), block_z) for g in gzs]
    my_line = ix * nz + iz

    for c, (first, count) in spans(FORWARD):
        part = pl.ds(first, count)

        def y_forward(a, carry, first=first):
            mid[a] = left_multiply(table_yf, thetas[first + a])
            return carry

        lax.fori_loop(0, count, y_forward, 0, unroll=True)
        rows = right_multiply(mid[pl.ds(0, count)].reshape(count * NY, NZ), tz, False)
        send1[part] = rows.reshape(count, 2, NY // 2, NZ)

        slot = FIRST_LINES + c
        for dx, dy, dz in ORDER:
            src = send1.at[part, :, gxs[dx] * nz + gzs[dz], quarter[dy]]
            to = {"gx": gxs[dx], "gy": gys[dy], "gz": gzs[dz]}
            send(src, recv1.at[part, :, me, :], slot, to)
        keep(send1.at[part, :, my_line, quarter[0]], recv1.at[part, :, me, :], slot)

    col = lax.broadcasted_iota(jnp.int32, (8, COLS), 1)
    wave_y = jnp.where(col < 128, my_line, my_line + NY // 2)
    wave_z = jnp.where(col < 128, col, col - 128) + iy * 128
    yz2 = wave_squared(wave_y, NY) + wave_squared(wave_z, NZ)
    top_sq = jnp.broadcast_to(q_top * q_top, (8, COLS))

    def gain_rows(r, carry):
        rows = pl.ds(pl.multiple_of(r * 8, 8), 8)
        k_sq = wave_squared(lax.broadcasted_iota(jnp.int32, (8, COLS), 0) + r * 8, NX) + yz2
        for s in range(SUMS):
            mass = top_sq * math.exp(-STEP * (2 * NQ - 2 - s))
            gain[s, rows, :] = LOCAL + mass / (k_sq + mass)
        return carry

    lax.fori_loop(0, NX // 8, gain_rows, 0)

    table_xf, table_xi = tx_f[...], tx_i[...]

    def over_y(src, dst, dy, slot):
        if dy:
            send(src, dst, slot, {"gy": gys[dy]})
        else:
            keep(src, dst, slot)

    def over_line(src, part, dx, dz, slot):
        dst = y_in.at[part, :, :, my_line, :]
        if dx or dz:
            send(src, dst, slot, {"gx": gxs[dx], "gz": gzs[dz]})
        else:
            keep(src, dst, slot)

    for c, (first, count) in spans(FORWARD):
        received(recv1.at[pl.ds(first, count)], FIRST_LINES + c)

        def x_forward(a, carry, first=first):
            lines = recv1[first + a]
            lines = jnp.concatenate([lines[0], lines[1]], axis=1)
            spec[first + a] = left_multiply(table_xf, lines)
            return carry

        lax.fori_loop(0, count, x_forward, 0, unroll=True)

    for c, (first, count) in spans(BACKWARD):
        part = pl.ds(first, count)

        def couple(r, carry, first=first, count=count):
            rows = pl.ds(pl.multiple_of(r * 8, 8), 8)
            for lane in range(COLS // 128):
                lanes = pl.ds(lane * 128, 128)
                source = [spec[b, rows, lanes] for b in range(NQ)]
                factor = {}
                for s in range(first, first + count + NQ - 1):
                    factor[s] = gain[s, rows, lanes]
                for a in range(count):
                    total = None
                    for b in range(NQ):
                        term = (coup[first + a, b] * factor[first + a + b]) * source[b]
                        total = term if total is None else total + term
                    prod[a, rows, lanes] = total
            return carry

        lax.fori_loop(0, NX // 8, couple, 0)

        def x_inverse(a, carry, first=first):
            lines = left_multiply(table_xi, prod[a])
            for r in range(2):
                send2[first + a, r] = lines[:, 128 * r : 128 * r + 128].reshape(4, NX // 4, 128)
            return carry

        lax.fori_loop(0, count, x_inverse, 0, unroll=True)

        slot = FIRST_BACK + 3 * c
        if ROUTES[c] == "P":
            for dx, dz in LINE_ORDER:
                src = send2.at[part, :, :, gzs[dz] * nx + gxs[dx], :]
                over_line(src, part, dx, dz, slot)
        else:
            for dy in (2, 1, 3, 0):
                src, dst = send2.at[part, :, gys[dy]], z_in_q.at[part, :, :, quarter[0]]
                over_y(src, dst, dy, slot)

    table_yi = ty_i[...]

    def y_inverse_all(first, count):
        def y_inverse(a, carry):
            planes_of = [
                jnp.concatenate([y_in[first + a, 0, k], y_in[first + a, 1, k]], axis=0)
                for k in range(4)
            ]
            rows = left_multiply(table_yi, jnp.concatenate(planes_of, axis=1))
            for k in range(4):
                y_out[first + a, k] = rows[:, 128 * k : 128 * k + 128]
            return carry

        lax.fori_loop(0, count, y_inverse, 0, unroll=True)

    def rows_for(dy):
        return pl.ds(pl.multiple_of(gys[dy] * block_y, 8), block_y)

    for c, (first, count) in spans(BACKWARD):
        part = pl.ds(first, count)
        slot = FIRST_BACK + 3 * c
        received((y_in if ROUTES[c] == "P" else z_in_q).at[part], slot)
        if ROUTES[c] == "P":
            y_inverse_all(first, count)
            for dy in (2, 1, 3, 0):
                src, dst = y_out.at[part, :, rows_for(dy), :], z_in_p.at[part, :, :, quarter[0]]
                over_y(src, dst, dy, slot + 1)
        else:
            rows = right_multiply(z_in_q[part].reshape(count * NY, NZ), tz, True)
            z_out_q[part] = rows.reshape(count, 2, 4, nx, NZ)
            for dx, dz in LINE_ORDER:
                z_of = z_part[dz]
                src = z_out_q.at[part, :, :, gxs[dx], z_of]
                over_line(src, part, dx, dz, slot + 1)

    for c, (first, count) in spans(BACKWARD):
        part = pl.ds(first, count)
        slot = FIRST_BACK + 3 * c
        received((z_in_p if ROUTES[c] == "P" else y_in).at[part], slot + 1)
        if ROUTES[c] == "P":
            rows = right_multiply(z_in_p[part].reshape(count * NY, NZ), tz, True)
            z_out_p[part] = rows.reshape(count, 4, block_y, NZ)
            for dz in (2, 3, 1, 0):
                src, dst = z_out_p.at[part, :, :, z_part[dz]], out.at[part, :, iz]
                if dz:
                    send(src, dst, slot + 2, {"gz": gzs[dz]})
                else:
                    keep(src, dst, slot + 2)
        else:
            y_inverse_all(first, count)
            for dy in (2, 1, 3, 0):
                over_y(y_out.at[part, :, rows_for(dy), :], out.at[part, iy], dy, slot + 2)

    for c, (first, count) in spans(BACKWARD):
        received(out.at[pl.ds(first, count)], FIRST_BACK + 3 * c + 2)

    sent(2 * (group - 1) * block_y * block_z // COLS, 0)
    pltpu.make_async_copy(others, others, ssem.at[1]).wait()
    pltpu.make_async_copy(far_others, far_others, ssem.at[2]).wait()
    for c, (_, count) in spans(FORWARD):
        sent((devices - 1) * count, FIRST_LINES + c)
    for c, (_, count) in spans(BACKWARD):
        few, many = 3 * 32 * count, (nx * nz - 1) * 4 * count
        for k, rows in enumerate((many, few, few) if ROUTES[c] == "P" else (few, many, few)):
            sent(rows, FIRST_BACK + 3 * c + k)


def write_out(fields, out, sem):
    copies = [pltpu.make_async_copy(fields.at[a], out.at[a], sem.at[a]) for a in range(NQ)]
    for copy in copies:
        copy.start()
    for copy in copies:
        copy.wait()


def solution(mesh):
    sizes = tuple(mesh.shape[axis] for axis in ("gx", "gy", "gz"))
    bz = basis(NZ)
    tz = np.stack(halves(bz))
    by, bx = basis(NY), basis(NX)
    x_rows = np.arange(NX).reshape(8, 4, 4).transpose(1, 2, 0).reshape(-1)
    tables = (tz, left_table(by.T), left_table(by), left_table(bx.T), left_table(bx[x_rows]))

    def body(density, coupling):
        vmem, hbm = (pl.BlockSpec(memory_space=space) for space in (pltpu.VMEM, pltpu.HBM))
        block = density.shape
        fields = pl.pallas_call(
            functools.partial(kernel, sizes),
            out_shape=jax.ShapeDtypeStruct((NQ, 4, block[0] // 4) + block[1:], F32),
            in_specs=[hbm] * (2 + len(tables)),
            out_specs=vmem,
            scratch_shapes=[
                pltpu.VMEM((block[0] + 4, block[1] + 16, block[2]), F32),
                pltpu.VMEM((block[2] + 16, block[0] * block[1]), F32),
                pltpu.VMEM((2, 2, block[0] * block[1]), F32),
                pltpu.VMEM((2, 2, block[0] * block[1]), F32),
                pltpu.VMEM((2, NY, NZ), F32),
                pltpu.VMEM(block, F32),
                pltpu.VMEM((2, 1, 128), F32),
                pltpu.VMEM((sizes[1] * sizes[2], 1, 128), F32),
                pltpu.VMEM((sizes[0], 1, 128), F32),
                pltpu.VMEM((NQ, NY, NZ), F32),
                pltpu.VMEM((max(FORWARD), NY, NZ), F32),
                pltpu.VMEM((NQ, 2, NY // 2, NZ), F32),
                pltpu.VMEM((NQ, 2, NX, 128), F32),
                pltpu.VMEM((NQ, NX, COLS), F32),
                pltpu.VMEM((SUMS, NX, COLS), F32),
                pltpu.VMEM((max(BACKWARD), NX, COLS), F32),
                pltpu.VMEM((NQ, 2, 4, NX // 4, 128), F32),
                pltpu.VMEM((NQ, 2, 4, NY // 2, 128), F32),
                pltpu.VMEM((NQ, 4, NY, 128), F32),
                pltpu.VMEM((NQ, 4, NY // 4, NZ), F32),
                pltpu.VMEM((NQ, 2, NX // 4, NZ), F32),
                pltpu.VMEM((NQ, 4, NY // 4, NZ), F32),
                pltpu.VMEM((NQ, 2, 4, NX // 16, NZ), F32),
                pltpu.VMEM(block, F32),
                pltpu.SMEM((NQ, NQ), F32),
                *[pltpu.VMEM(table.shape, BF16) for table in tables],
                pltpu.SemaphoreType.DMA((2 + len(tables),)),
                pltpu.SemaphoreType.DMA((SLOTS,)),
                pltpu.SemaphoreType.DMA((SLOTS,)),
                pltpu.SemaphoreType.DMA((8,)),
                pltpu.SemaphoreType.DMA((8,)),
            ],
            compiler_params=pltpu.CompilerParams(
                collective_id=0, has_side_effects=True, vmem_limit_bytes=40 * 1024 * 1024
            ),
            name="convolve",
        )(*[pltpu.with_memory_space_constraint(x, pltpu.HBM) for x in (density, coupling, *map(jnp.asarray, tables))])
        return pl.pallas_call(
            write_out,
            out_shape=jax.ShapeDtypeStruct((NQ,) + block, F32),
            in_specs=[vmem],
            out_specs=hbm,
            scratch_shapes=[pltpu.SemaphoreType.DMA((NQ,))],
            compiler_params=pltpu.CompilerParams(vmem_limit_bytes=4 * 1024 * 1024),
            cost_estimate=pl.CostEstimate(flops=0, bytes_accessed=8 * NQ * density.size, transcendentals=0),
            name="write_out",
        )(fields.reshape((NQ,) + block))

    placed = (P("gx", "gy", "gz"), P())
    return jax.shard_map(
        body, mesh=mesh, in_specs=placed, out_specs=P(None, "gx", "gy", "gz"), check_vma=False
    )
```

```python
import functools
import math

import jax
import jax.numpy as jnp
import numpy as np
from jax import lax
from jax.experimental import pallas as pl
from jax.experimental.pallas import tpu as pltpu
from jax.sharding import PartitionSpec as P

MESH = pl.DeviceIdType.MESH
F32 = jnp.float32
BF16 = jnp.bfloat16

NQ = 14
NX, NY, NZ = 128, 64, 512
FORWARD = (3, 5, 6)
BACKWARD = (2, 3, 3, 3, 3)
ROUTES = "PQPQP"
LAG = 5
KNOTS = NQ + 2
COLS = NY * NZ // NX
SUMS = 2 * NQ - 1

ZAB = 0.8491 / 9.0
Q_CUT = 5.0
STEP = 0.07
LOCAL = 0.25
LAM = math.sqrt(3.0) - 2.0
FIRST_LINES, FIRST_BACK = 3, 3 + len(FORWARD)
SLOTS = FIRST_BACK + 3 * len(BACKWARD)


def frequencies(length):
    half = length // 2
    return np.array(list(range(half + 1)) + list(range(1, half)), dtype=np.float64)


def basis(length):
    half = length // 2
    points = np.arange(length)[:, None]
    waves = frequencies(length)[None, :]
    angle = 2.0 * np.pi / length * np.mod(points * waves, length)
    table = np.where(np.arange(length)[None, :] <= half, np.cos(angle), np.sin(angle))
    scale = np.full((1, length), math.sqrt(2.0 / length))
    scale[0, 0] = scale[0, half] = math.sqrt(1.0 / length)
    return table * scale


def spans(counts):
    starts = [sum(counts[:k]) for k in range(len(counts))]
    return list(enumerate(zip(starts, counts)))


def hops(offset):
    dx, dy, dz = offset
    along_y = (0, 1, 2, 1)[dx // 4 * 2 + dz // 2]
    return min(dy, 4 - dy) + min(dx % 4, 4 - dx % 4) + along_y


def far_first():
    offsets = [(dx, dy, dz) for dx in range(8) for dy in range(4) for dz in range(4)][1:]
    shuffled = [offsets[k] for k in np.random.RandomState(3).permutation(len(offsets))]
    return sorted(shuffled, key=lambda offset: -hops(offset))


ORDER = far_first()
LINE_ORDER = [(dx, dz) for dx, dy, dz in ORDER if dy == 0] + [(0, 0)]


def halves(table):
    high = table.astype(BF16)
    low = (table - high.astype(np.float64)).astype(BF16)
    return high, low


def left_table(table):
    high, low = halves(table)
    return np.concatenate([high, high, low], axis=1)


def wave_squared(index, length):
    wave = jnp.where(index <= length // 2, index, index - length // 2).astype(F32)
    wave = wave * (2.0 * math.pi / length)
    return wave * wave


def split(value):
    high = value.astype(BF16)
    return high, (value - high.astype(F32)).astype(BF16)


def left_multiply(table, value):
    high, low = split(value)
    return jnp.dot(table, jnp.concatenate([high, low, high], axis=0), preferred_element_type=F32)


def right_multiply(value, table_ref, transposed):
    high, low = split(value)
    rows = jnp.concatenate([high, low, high], axis=1)
    side = 1 if transposed else 0
    weights = jnp.concatenate([table_ref[0], table_ref[0], table_ref[1]], axis=side)
    return lax.dot_general(rows, weights, (((1,), (side,)), ((), ())), preferred_element_type=F32)


def kernel(
    sizes, dens_in, coup_in, tz_in, ty_f_in, ty_i_in, tx_f_in, tx_i_in, out,
    ext, zext, zsend, zhalo, planes, q_buf, top_src, near_tops, far_tops, thetas, mid, send1, recv1, spec, gain, prod, send2, y_in, y_out, z_in_p, z_in_q, z_out_p, z_out_q,
    dens, coup, tz, ty_f, ty_i, tx_f, tx_i, load_sem, ssem, rsem, hsend, hrecv,
):
    devices = NX
    nx, ny, nz = sizes
    group = ny * nz
    ix, iy, iz = lax.axis_index("gx"), lax.axis_index("gy"), lax.axis_index("gz")
    me = (ix * ny + iy) * nz + iz
    block_x, block_y, block_z = NX // nx, NY // ny, NZ // nz

    def send(src, dst, slot, to):
        pltpu.make_async_remote_copy(
            src, dst, ssem.at[slot], rsem.at[slot], device_id=to, device_id_type=MESH
        ).start()

    def keep(src, dst, slot):
        pltpu.make_async_copy(src, dst, rsem.at[slot]).start()

    def received(ref, slot):
        pltpu.make_async_copy(ref, ref, rsem.at[slot]).wait()

    def sent(rows, slot):
        full, rest = divmod(rows, NX)
        if full:
            part = spec.at[pl.ds(0, full)]
            pltpu.make_async_copy(part, part, ssem.at[slot]).wait()
        if rest // 8:
            part = spec.at[0, pl.ds(0, rest // 8 * 8)]
            pltpu.make_async_copy(part, part, ssem.at[slot]).wait()
        for _ in range(rest % 8):
            part = spec.at[0, 0]
            pltpu.make_async_copy(part, part, ssem.at[slot]).wait()

    inputs = ((dens_in, dens), (coup_in, coup), (tz_in, tz), (ty_f_in, ty_f), (ty_i_in, ty_i))
    inputs = inputs + ((tx_f_in, tx_f), (tx_i_in, tx_i))
    loads = [pltpu.make_async_copy(a, b, load_sem.at[k]) for k, (a, b) in enumerate(inputs)]
    for load in loads:
        load.start()
    z_len = nx // 2
    y_hi, z_at, y_lo, core = lax.div(ix, z_len), lax.rem(ix, z_len), lax.div(iz, 2), lax.rem(iz, 2)
    gys = [lax.rem(iy + j, ny) for j in range(ny)]
    gzs = [
        (1 - y_lo if j // 2 else y_lo) * 2 + (1 - core if j % 2 else core) for j in range(nz)
    ]
    gxs = [
        (1 - y_hi if j // z_len else y_hi) * z_len + lax.rem(z_at + j % z_len, z_len)
        for j in range(nx)
    ]
    near = [(dy, dz) for dz in range(nz) for dy in range(ny)]
    barrier = pltpu.get_barrier_semaphore()
    for dy, dz in near[1:]:
        pl.semaphore_signal(
            barrier, inc=1, device_id={"gy": gys[dy], "gz": gzs[dz]}, device_id_type=MESH
        )
    for dx in range(1, nx):
        pl.semaphore_signal(
            barrier, inc=1, device_id={"gx": gxs[dx]}, device_id_type=MESH
        )
    loads[0].wait()
    block = dens[...]
    ext[pl.ds(2, block_x), pl.ds(8, block_y), :] = block
    turned = block.reshape(block_x * block_y, block_z).T
    zext[pl.ds(8, block_z), :] = turned
    zsend[0] = turned[:2]
    zsend[1] = turned[block_z - 2 :]
    pl.semaphore_wait(barrier, group - 1 + nx - 1)

    halos = []

    def halo(src, dst, to):
        slot = len(halos)
        copy = pltpu.make_async_remote_copy(
            src, dst, hsend.at[slot], hrecv.at[slot], device_id=to, device_id_type=MESH
        )
        copy.start()
        halos.append(copy)

    low_x, high_x = {"gx": lax.rem(ix + nx - 1, nx)}, {"gx": lax.rem(ix + 1, nx)}
    low_y, high_y = {"gy": gys[ny - 1]}, {"gy": gys[1]}
    low_z, high_z = {"gz": lax.rem(iz + nz - 1, nz)}, {"gz": lax.rem(iz + 1, nz)}
    inner_x, inner_y = pl.ds(2, block_x), pl.ds(8, block_y)
    halo(dens.at[pl.ds(0, 2)], ext.at[pl.ds(block_x + 2, 2), inner_y], low_x)
    halo(dens.at[pl.ds(block_x - 2, 2)], ext.at[pl.ds(0, 2), inner_y], high_x)
    for k in range(2):
        halo(dens.at[:, k, :], ext.at[inner_x, block_y + 8 + k, :], low_y)
        halo(dens.at[:, block_y - 2 + k, :], ext.at[inner_x, 6 + k, :], high_y)
    halo(zsend.at[0], zhalo.at[1], low_z)
    halo(zsend.at[1], zhalo.at[0], high_z)

    here, row_x = iy * nz + iz, iy * nz + iz
    here_y = pl.ds(pl.multiple_of(iy * block_y, 8), block_y)
    here_z = pl.ds(pl.multiple_of(iz * block_z, 128), block_z)

    def rows_out(src, which):
        for dy, dz in near:
            row = gys[dy] * nz + gzs[dz]
            dst = planes.at[which, here_y, here_z]
            if dy or dz:
                send(src.at[row], dst, 0, {"gy": gys[dy], "gz": gzs[dz]})
            else:
                keep(src.at[row], dst, 0)

    for copy in halos:
        copy.wait()

    zext[6:8, :] = zhalo[0]
    zext[pl.ds(block_z + 8, 2), :] = zhalo[1]

    def squared_slope(at):
        slope = (8.0 * (at(1) - at(-1)) - (at(2) - at(-2))) / 12.0
        return slope * slope

    grad_sq = squared_slope(lambda o: ext[pl.ds(2 + o, block_x), inner_y, :])
    grad_sq = grad_sq + squared_slope(lambda o: ext[inner_x, pl.ds(8 + o, block_y), :])
    along_z = squared_slope(lambda o: zext[pl.ds(8 + o, block_z), :])
    grad_sq = grad_sq + along_z.T.reshape(block_x, block_y, block_z)
    cube = (3.0 * math.pi * math.pi) * block
    fermi_k = jnp.exp(jnp.log(cube) / 3.0)
    fermi_k = fermi_k - (fermi_k - cube / (fermi_k * fermi_k)) * (1.0 / 3.0)
    reduced = grad_sq / (4.0 * fermi_k * fermi_k * block * block)
    scaled = fermi_k * (1.0 + ZAB * reduced) / Q_CUT
    series = jnp.full_like(scaled, 1.0 / 12.0)
    for order in range(11, 0, -1):
        series = series * scaled + 1.0 / order
    q_zero = Q_CUT * (1.0 - jnp.exp(-(series * scaled)))
    q_buf[...] = q_zero
    top = jnp.max(jnp.max(q_zero, axis=0), axis=0, keepdims=True)
    top = jnp.broadcast_to(jnp.max(top, axis=1, keepdims=True), (1, 128))
    top_src[0] = top
    near_tops[here] = top

    for dy, dz in near[1:]:
        send(top_src.at[0], near_tops.at[here], 1, {"gy": gys[dy], "gz": gzs[dz]})
    rows_out(q_buf, 1)
    rows_out(dens, 0)
    others = near_tops.at[pl.ds(0, group - 1)]
    received(others, 1)
    top = jnp.max(near_tops[...], axis=0)
    top_src[1] = top
    far_tops[ix] = top
    for dx in range(1, nx):
        send(top_src.at[1], far_tops.at[ix], 2, {"gx": gxs[dx]})
    far_others = far_tops.at[pl.ds(0, nx - 1)]
    received(far_others, 2)
    q_top = jnp.max(far_tops[...])
    received(planes, 0)

    inv_top = 1.0 / jnp.broadcast_to(q_top, (8, 128))
    weight = math.sqrt(3.0) / 6.0

    def theta_rows(r, carry):
        rows = pl.ds(pl.multiple_of(r * 8, 8), 8)
        for lane in range(NZ // 128):
            lanes = pl.ds(lane * 128, 128)
            value = planes[0, rows, lanes] * weight
            position = jnp.maximum(
                (NQ - 1.0) + jnp.log(planes[1, rows, lanes] * inv_top) / STEP, 0.0
            )
            splines = []
            for j in range(-1, NQ + 1):
                offset = jnp.abs(position - float(j))
                wide = jnp.maximum(2.0 - offset, 0.0)
                narrow = jnp.maximum(1.0 - offset, 0.0)
                splines.append(wide * wide * wide - 4.0 * (narrow * narrow * narrow))
            up = [splines[0]]
            for j in range(1, KNOTS - 1):
                up.append(splines[j] + LAM * up[-1])
            down = splines[KNOTS - 1]
            for a in range(NQ - 1, -1, -1):
                below = LAM * down
                thetas[a, rows, lanes] = (up[a + 1] + below) * value
                down = splines[a + 1] + below
        return carry

    lax.fori_loop(0, NY // 8, theta_rows, 0)

    for load in loads[1:]:
        load.wait()
    table_yf = ty_f[...]
    quarter = [pl.ds(pl.multiple_of(g * 128, 128), 128) for g in gys]
    z_part = [pl.ds(pl.multiple_of(g * block_z, 128), block_z) for g in gzs]
    my_line = ix * nz + iz

    for c, (first, count) in spans(FORWARD):
        part = pl.ds(first, count)

        def y_forward(a, carry, first=first):
            mid[a] = left_multiply(table_yf, thetas[first + a])
            return carry

        lax.fori_loop(0, count, y_forward, 0, unroll=True)
        rows = right_multiply(mid[pl.ds(0, count)].reshape(count * NY, NZ), tz, False)
        send1[part] = rows.reshape(count, 2, NY // 2, NZ)

        slot = FIRST_LINES + c
        for dx, dy, dz in ORDER:
            src = send1.at[part, :, gxs[dx] * nz + gzs[dz], quarter[dy]]
            to = {"gx": gxs[dx], "gy": gys[dy], "gz": gzs[dz]}
            send(src, recv1.at[part, :, me, :], slot, to)
        keep(send1.at[part, :, my_line, quarter[0]], recv1.at[part, :, me, :], slot)

    col = lax.broadcasted_iota(jnp.int32, (8, COLS), 1)
    wave_y = jnp.where(col < 128, my_line, my_line + NY // 2)
    wave_z = jnp.where(col < 128, col, col - 128) + iy * 128
    yz2 = wave_squared(wave_y, NY) + wave_squared(wave_z, NZ)
    top_sq = jnp.broadcast_to(q_top * q_top, (8, COLS))

    def gain_rows(r, carry):
        rows = pl.ds(pl.multiple_of(r * 8, 8), 8)
        k_sq = wave_squared(lax.broadcasted_iota(jnp.int32, (8, COLS), 0) + r * 8, NX) + yz2
        for s in range(SUMS):
            mass = top_sq * math.exp(-STEP * (2 * NQ - 2 - s))
            gain[s, rows, :] = LOCAL + mass / (k_sq + mass)
        return carry

    lax.fori_loop(0, NX // 8, gain_rows, 0)

    table_xf, table_xi = tx_f[...], tx_i[...]

    def over_y(src, dst, dy, slot):
        if dy:
            send(src, dst, slot, {"gy": gys[dy]})
        else:
            keep(src, dst, slot)

    def over_line(src, part, dx, dz, slot):
        dst = y_in.at[part, :, :, my_line, :]
        if dx or dz:
            send(src, dst, slot, {"gx": gxs[dx], "gz": gzs[dz]})
        else:
            keep(src, dst, slot)

    for c, (first, count) in spans(FORWARD):
        received(recv1.at[pl.ds(first, count)], FIRST_LINES + c)

        def x_forward(a, carry, first=first):
            lines = recv1[first + a]
            lines = jnp.concatenate([lines[0], lines[1]], axis=1)
            spec[first + a] = left_multiply(table_xf, lines)
            return carry

        lax.fori_loop(0, count, x_forward, 0, unroll=True)

    for c, (first, count) in spans(BACKWARD):
        part = pl.ds(first, count)

        def couple(r, carry, first=first, count=count):
            rows = pl.ds(pl.multiple_of(r * 8, 8), 8)
            for lane in range(COLS // 128):
                lanes = pl.ds(lane * 128, 128)
                source = [spec[b, rows, lanes] for b in range(NQ)]
                factor = {}
                for s in range(first, first + count + NQ - 1):
                    factor[s] = gain[s, rows, lanes]
                for a in range(count):
                    total = None
                    for b in range(NQ):
                        term = (coup[first + a, b] * factor[first + a + b]) * source[b]
                        total = term if total is None else total + term
                    prod[a, rows, lanes] = total
            return carry

        lax.fori_loop(0, NX // 8, couple, 0)

        def x_inverse(a, carry, first=first):
            lines = left_multiply(table_xi, prod[a])
            for r in range(2):
                send2[first + a, r] = lines[:, 128 * r : 128 * r + 128].reshape(4, NX // 4, 128)
            return carry

        lax.fori_loop(0, count, x_inverse, 0, unroll=True)

        slot = FIRST_BACK + 3 * c
        if ROUTES[c] == "P":
            for dx, dz in LINE_ORDER:
                src = send2.at[part, :, :, gzs[dz] * nx + gxs[dx], :]
                over_line(src, part, dx, dz, slot)
        else:
            for dy in (2, 1, 3, 0):
                src, dst = send2.at[part, :, gys[dy]], z_in_q.at[part, :, :, quarter[0]]
                over_y(src, dst, dy, slot)

    table_yi = ty_i[...]

    def y_inverse_all(first, count):
        def y_inverse(a, carry):
            planes_of = [
                jnp.concatenate([y_in[first + a, 0, k], y_in[first + a, 1, k]], axis=0)
                for k in range(4)
            ]
            rows = left_multiply(table_yi, jnp.concatenate(planes_of, axis=1))
            for k in range(4):
                y_out[first + a, k] = rows[:, 128 * k : 128 * k + 128]
            return carry

        lax.fori_loop(0, count, y_inverse, 0, unroll=True)

    def rows_for(dy):
        return pl.ds(pl.multiple_of(gys[dy] * block_y, 8), block_y)

    def middle(c, first, count):
        part = pl.ds(first, count)
        slot = FIRST_BACK + 3 * c
        received((y_in if ROUTES[c] == "P" else z_in_q).at[part], slot)
        if ROUTES[c] == "P":
            y_inverse_all(first, count)
            for dy in (2, 1, 3, 0):
                src, dst = y_out.at[part, :, rows_for(dy), :], z_in_p.at[part, :, :, quarter[0]]
                over_y(src, dst, dy, slot + 1)
        else:
            rows = right_multiply(z_in_q[part].reshape(count * NY, NZ), tz, True)
            z_out_q[part] = rows.reshape(count, 2, 4, nx, NZ)
            for dx, dz in LINE_ORDER:
                z_of = z_part[dz]
                src = z_out_q.at[part, :, :, gxs[dx], z_of]
                over_line(src, part, dx, dz, slot + 1)

    def last(c, first, count):
        part = pl.ds(first, count)
        slot = FIRST_BACK + 3 * c
        received((z_in_p if ROUTES[c] == "P" else y_in).at[part], slot + 1)
        if ROUTES[c] == "P":
            rows = right_multiply(z_in_p[part].reshape(count * NY, NZ), tz, True)
            z_out_p[part] = rows.reshape(count, 4, block_y, NZ)
            for dz in (2, 3, 1, 0):
                src, dst = z_out_p.at[part, :, :, z_part[dz]], out.at[part, :, iz]
                if dz:
                    send(src, dst, slot + 2, {"gz": gzs[dz]})
                else:
                    keep(src, dst, slot + 2)
        else:
            y_inverse_all(first, count)
            for dy in (2, 1, 3, 0):
                over_y(y_out.at[part, :, rows_for(dy), :], out.at[part, iy], dy, slot + 2)

    chunks = spans(BACKWARD)
    for k in range(len(chunks) + LAG):
        if k < len(chunks):
            c, (first, count) = chunks[k]
            middle(c, first, count)
        if k >= LAG:
            c, (first, count) = chunks[k - LAG]
            last(c, first, count)

    for c, (first, count) in spans(BACKWARD):
        received(out.at[pl.ds(first, count)], FIRST_BACK + 3 * c + 2)

    sent(2 * (group - 1) * block_y * block_z // COLS, 0)
    pltpu.make_async_copy(others, others, ssem.at[1]).wait()
    pltpu.make_async_copy(far_others, far_others, ssem.at[2]).wait()
    for c, (_, count) in spans(FORWARD):
        sent((devices - 1) * count, FIRST_LINES + c)
    for c, (_, count) in spans(BACKWARD):
        few, many = 3 * 32 * count, (nx * nz - 1) * 4 * count
        for k, rows in enumerate((many, few, few) if ROUTES[c] == "P" else (few, many, few)):
            sent(rows, FIRST_BACK + 3 * c + k)


def write_out(fields, out, sem):
    copies = [pltpu.make_async_copy(fields.at[a], out.at[a], sem.at[a]) for a in range(NQ)]
    for copy in copies:
        copy.start()
    for copy in copies:
        copy.wait()


def solution(mesh):
    sizes = tuple(mesh.shape[axis] for axis in ("gx", "gy", "gz"))
    bz = basis(NZ)
    tz = np.stack(halves(bz))
    by, bx = basis(NY), basis(NX)
    x_rows = np.arange(NX).reshape(8, 4, 4).transpose(1, 2, 0).reshape(-1)
    tables = (tz, left_table(by.T), left_table(by), left_table(bx.T), left_table(bx[x_rows]))

    def body(density, coupling):
        vmem, hbm = (pl.BlockSpec(memory_space=space) for space in (pltpu.VMEM, pltpu.HBM))
        block = density.shape
        fields = pl.pallas_call(
            functools.partial(kernel, sizes),
            out_shape=jax.ShapeDtypeStruct((NQ, 4, block[0] // 4) + block[1:], F32),
            in_specs=[hbm] * (2 + len(tables)),
            out_specs=vmem,
            scratch_shapes=[
                pltpu.VMEM((block[0] + 4, block[1] + 16, block[2]), F32),
                pltpu.VMEM((block[2] + 16, block[0] * block[1]), F32),
                pltpu.VMEM((2, 2, block[0] * block[1]), F32),
                pltpu.VMEM((2, 2, block[0] * block[1]), F32),
                pltpu.VMEM((2, NY, NZ), F32),
                pltpu.VMEM(block, F32),
                pltpu.VMEM((2, 1, 128), F32),
                pltpu.VMEM((sizes[1] * sizes[2], 1, 128), F32),
                pltpu.VMEM((sizes[0], 1, 128), F32),
                pltpu.VMEM((NQ, NY, NZ), F32),
                pltpu.VMEM((max(FORWARD), NY, NZ), F32),
                pltpu.VMEM((NQ, 2, NY // 2, NZ), F32),
                pltpu.VMEM((NQ, 2, NX, 128), F32),
                pltpu.VMEM((NQ, NX, COLS), F32),
                pltpu.VMEM((SUMS, NX, COLS), F32),
                pltpu.VMEM((max(BACKWARD), NX, COLS), F32),
                pltpu.VMEM((NQ, 2, 4, NX // 4, 128), F32),
                pltpu.VMEM((NQ, 2, 4, NY // 2, 128), F32),
                pltpu.VMEM((NQ, 4, NY, 128), F32),
                pltpu.VMEM((NQ, 4, NY // 4, NZ), F32),
                pltpu.VMEM((NQ, 2, NX // 4, NZ), F32),
                pltpu.VMEM((NQ, 4, NY // 4, NZ), F32),
                pltpu.VMEM((NQ, 2, 4, NX // 16, NZ), F32),
                pltpu.VMEM(block, F32),
                pltpu.SMEM((NQ, NQ), F32),
                *[pltpu.VMEM(table.shape, BF16) for table in tables],
                pltpu.SemaphoreType.DMA((2 + len(tables),)),
                pltpu.SemaphoreType.DMA((SLOTS,)),
                pltpu.SemaphoreType.DMA((SLOTS,)),
                pltpu.SemaphoreType.DMA((8,)),
                pltpu.SemaphoreType.DMA((8,)),
            ],
            compiler_params=pltpu.CompilerParams(
                collective_id=0, has_side_effects=True, vmem_limit_bytes=40 * 1024 * 1024
            ),
            name="convolve",
        )(*[pltpu.with_memory_space_constraint(x, pltpu.HBM) for x in (density, coupling, *map(jnp.asarray, tables))])
        return pl.pallas_call(
            write_out,
            out_shape=jax.ShapeDtypeStruct((NQ,) + block, F32),
            in_specs=[vmem],
            out_specs=hbm,
            scratch_shapes=[pltpu.SemaphoreType.DMA((NQ,))],
            compiler_params=pltpu.CompilerParams(vmem_limit_bytes=4 * 1024 * 1024),
            cost_estimate=pl.CostEstimate(flops=0, bytes_accessed=8 * NQ * density.size, transcendentals=0),
            name="write_out",
        )(fields.reshape((NQ,) + block))

    placed = (P("gx", "gy", "gz"), P())
    return jax.shard_map(
        body, mesh=mesh, in_specs=placed, out_specs=P(None, "gx", "gy", "gz"), check_vma=False
    )
```

```python
import functools
import math

import jax
import jax.numpy as jnp
import numpy as np
from jax import lax
from jax.experimental import pallas as pl
from jax.experimental.pallas import tpu as pltpu
from jax.sharding import PartitionSpec as P

MESH = pl.DeviceIdType.MESH
F32 = jnp.float32
BF16 = jnp.bfloat16

NQ = 14
NX, NY, NZ = 128, 64, 512
FORWARD = (3, 5, 6)
BACKWARD = (2, 3, 3, 3, 3)
ROUTES = "PQPQP"
LAG = 5
KNOTS = NQ + 2
COLS = NY * NZ // NX
SUMS = 2 * NQ - 1

ZAB = 0.8491 / 9.0
Q_CUT = 5.0
STEP = 0.07
LOCAL = 0.25
LAM = math.sqrt(3.0) - 2.0
FIRST_LINES, FIRST_BACK = 3, 3 + len(FORWARD)
SLOTS = FIRST_BACK + 3 * len(BACKWARD)


def frequencies(length):
    half = length // 2
    return np.array(list(range(half + 1)) + list(range(1, half)), dtype=np.float64)


def basis(length):
    half = length // 2
    points = np.arange(length)[:, None]
    waves = frequencies(length)[None, :]
    angle = 2.0 * np.pi / length * np.mod(points * waves, length)
    table = np.where(np.arange(length)[None, :] <= half, np.cos(angle), np.sin(angle))
    scale = np.full((1, length), math.sqrt(2.0 / length))
    scale[0, 0] = scale[0, half] = math.sqrt(1.0 / length)
    return table * scale


def spans(counts):
    starts = [sum(counts[:k]) for k in range(len(counts))]
    return list(enumerate(zip(starts, counts)))


def hops(offset):
    dx, dy, dz = offset
    along_y = (0, 1, 2, 1)[dx // 4 * 2 + dz // 2]
    return min(dy, 4 - dy) + min(dx % 4, 4 - dx % 4) + along_y


def far_first():
    offsets = [(dx, dy, dz) for dx in range(8) for dy in range(4) for dz in range(4)][1:]
    shuffled = [offsets[k] for k in np.random.RandomState(3).permutation(len(offsets))]
    return sorted(shuffled, key=lambda offset: -hops(offset))


ORDER = far_first()
LINE_ORDER = [(dx, dz) for dx, dy, dz in ORDER if dy == 0] + [(0, 0)]


def halves(table):
    high = table.astype(BF16)
    low = (table - high.astype(np.float64)).astype(BF16)
    return high, low


def left_table(table):
    high, low = halves(table)
    return np.concatenate([high, high, low], axis=1)


def wave_squared(index, length):
    wave = jnp.where(index <= length // 2, index, index - length // 2).astype(F32)
    wave = wave * (2.0 * math.pi / length)
    return wave * wave


def split(value):
    high = value.astype(BF16)
    return high, (value - high.astype(F32)).astype(BF16)


def left_multiply(table, value):
    high, low = split(value)
    return jnp.dot(table, jnp.concatenate([high, low, high], axis=0), preferred_element_type=F32)


def right_multiply(value, table_ref, transposed):
    high, low = split(value)
    rows = jnp.concatenate([high, low, high], axis=1)
    side = 1 if transposed else 0
    weights = jnp.concatenate([table_ref[0], table_ref[0], table_ref[1]], axis=side)
    return lax.dot_general(rows, weights, (((1,), (side,)), ((), ())), preferred_element_type=F32)


def kernel(
    sizes, dens_in, coup_in, tz_in, ty_f_in, ty_i_in, tx_f_in, tx_i_in, out,
    ext, zext, zsend, zhalo, planes, q_buf, top_src, near_tops, far_tops, thetas, mid, send1, recv1, spec, gain, link, prod, send2, y_in, y_out, z_in_p, z_in_q, z_out_p, z_out_q,
    dens, coup, tz, ty_f, ty_i, tx_f, tx_i, load_sem, ssem, rsem, hsend, hrecv,
):
    devices = NX
    nx, ny, nz = sizes
    group = ny * nz
    ix, iy, iz = lax.axis_index("gx"), lax.axis_index("gy"), lax.axis_index("gz")
    me = (ix * ny + iy) * nz + iz
    block_x, block_y, block_z = NX // nx, NY // ny, NZ // nz

    def send(src, dst, slot, to):
        pltpu.make_async_remote_copy(
            src, dst, ssem.at[slot], rsem.at[slot], device_id=to, device_id_type=MESH
        ).start()

    def keep(src, dst, slot):
        pltpu.make_async_copy(src, dst, rsem.at[slot]).start()

    def received(ref, slot):
        pltpu.make_async_copy(ref, ref, rsem.at[slot]).wait()

    def sent(rows, slot):
        full, rest = divmod(rows, NX)
        if full:
            part = spec.at[pl.ds(0, full)]
            pltpu.make_async_copy(part, part, ssem.at[slot]).wait()
        if rest // 8:
            part = spec.at[0, pl.ds(0, rest // 8 * 8)]
            pltpu.make_async_copy(part, part, ssem.at[slot]).wait()
        for _ in range(rest % 8):
            part = spec.at[0, 0]
            pltpu.make_async_copy(part, part, ssem.at[slot]).wait()

    inputs = ((dens_in, dens), (coup_in, coup), (tz_in, tz), (ty_f_in, ty_f), (ty_i_in, ty_i))
    inputs = inputs + ((tx_f_in, tx_f), (tx_i_in, tx_i))
    loads = [pltpu.make_async_copy(a, b, load_sem.at[k]) for k, (a, b) in enumerate(inputs)]
    for load in loads:
        load.start()
    z_len = nx // 2
    y_hi, z_at, y_lo, core = lax.div(ix, z_len), lax.rem(ix, z_len), lax.div(iz, 2), lax.rem(iz, 2)
    gys = [lax.rem(iy + j, ny) for j in range(ny)]
    gzs = [
        (1 - y_lo if j // 2 else y_lo) * 2 + (1 - core if j % 2 else core) for j in range(nz)
    ]
    gxs = [
        (1 - y_hi if j // z_len else y_hi) * z_len + lax.rem(z_at + j % z_len, z_len)
        for j in range(nx)
    ]
    near = [(dy, dz) for dz in range(nz) for dy in range(ny)]
    barrier = pltpu.get_barrier_semaphore()
    for dy, dz in near[1:]:
        pl.semaphore_signal(
            barrier, inc=1, device_id={"gy": gys[dy], "gz": gzs[dz]}, device_id_type=MESH
        )
    for dx in range(1, nx):
        pl.semaphore_signal(
            barrier, inc=1, device_id={"gx": gxs[dx]}, device_id_type=MESH
        )
    loads[0].wait()
    block = dens[...]
    ext[pl.ds(2, block_x), pl.ds(8, block_y), :] = block
    turned = block.reshape(block_x * block_y, block_z).T
    zext[pl.ds(8, block_z), :] = turned
    zsend[0] = turned[:2]
    zsend[1] = turned[block_z - 2 :]
    pl.semaphore_wait(barrier, group - 1 + nx - 1)

    halos = []

    def halo(src, dst, to):
        slot = len(halos)
        copy = pltpu.make_async_remote_copy(
            src, dst, hsend.at[slot], hrecv.at[slot], device_id=to, device_id_type=MESH
        )
        copy.start()
        halos.append(copy)

    low_x, high_x = {"gx": lax.rem(ix + nx - 1, nx)}, {"gx": lax.rem(ix + 1, nx)}
    low_y, high_y = {"gy": gys[ny - 1]}, {"gy": gys[1]}
    low_z, high_z = {"gz": lax.rem(iz + nz - 1, nz)}, {"gz": lax.rem(iz + 1, nz)}
    inner_x, inner_y = pl.ds(2, block_x), pl.ds(8, block_y)
    halo(dens.at[pl.ds(0, 2)], ext.at[pl.ds(block_x + 2, 2), inner_y], low_x)
    halo(dens.at[pl.ds(block_x - 2, 2)], ext.at[pl.ds(0, 2), inner_y], high_x)
    for k in range(2):
        halo(dens.at[:, k, :], ext.at[inner_x, block_y + 8 + k, :], low_y)
        halo(dens.at[:, block_y - 2 + k, :], ext.at[inner_x, 6 + k, :], high_y)
    halo(zsend.at[0], zhalo.at[1], low_z)
    halo(zsend.at[1], zhalo.at[0], high_z)

    here, row_x = iy * nz + iz, iy * nz + iz
    here_y = pl.ds(pl.multiple_of(iy * block_y, 8), block_y)
    here_z = pl.ds(pl.multiple_of(iz * block_z, 128), block_z)

    def rows_out(src, which):
        for dy, dz in near:
            row = gys[dy] * nz + gzs[dz]
            dst = planes.at[which, here_y, here_z]
            if dy or dz:
                send(src.at[row], dst, 0, {"gy": gys[dy], "gz": gzs[dz]})
            else:
                keep(src.at[row], dst, 0)

    for copy in halos:
        copy.wait()

    zext[6:8, :] = zhalo[0]
    zext[pl.ds(block_z + 8, 2), :] = zhalo[1]

    def squared_slope(at):
        slope = (8.0 * (at(1) - at(-1)) - (at(2) - at(-2))) / 12.0
        return slope * slope

    grad_sq = squared_slope(lambda o: ext[pl.ds(2 + o, block_x), inner_y, :])
    grad_sq = grad_sq + squared_slope(lambda o: ext[inner_x, pl.ds(8 + o, block_y), :])
    along_z = squared_slope(lambda o: zext[pl.ds(8 + o, block_z), :])
    grad_sq = grad_sq + along_z.T.reshape(block_x, block_y, block_z)
    cube = (3.0 * math.pi * math.pi) * block
    fermi_k = jnp.exp(jnp.log(cube) / 3.0)
    fermi_k = fermi_k - (fermi_k - cube / (fermi_k * fermi_k)) * (1.0 / 3.0)
    reduced = grad_sq / (4.0 * fermi_k * fermi_k * block * block)
    scaled = fermi_k * (1.0 + ZAB * reduced) / Q_CUT
    series = jnp.full_like(scaled, 1.0 / 12.0)
    for order in range(11, 0, -1):
        series = series * scaled + 1.0 / order
    q_zero = Q_CUT * (1.0 - jnp.exp(-(series * scaled)))
    q_buf[...] = q_zero
    top = jnp.max(jnp.max(q_zero, axis=0), axis=0, keepdims=True)
    top = jnp.broadcast_to(jnp.max(top, axis=1, keepdims=True), (1, 128))
    top_src[0] = top
    near_tops[here] = top

    for dy, dz in near[1:]:
        send(top_src.at[0], near_tops.at[here], 1, {"gy": gys[dy], "gz": gzs[dz]})
    rows_out(q_buf, 1)
    rows_out(dens, 0)
    others = near_tops.at[pl.ds(0, group - 1)]
    received(others, 1)
    top = jnp.max(near_tops[...], axis=0)
    top_src[1] = top
    far_tops[ix] = top
    for dx in range(1, nx):
        send(top_src.at[1], far_tops.at[ix], 2, {"gx": gxs[dx]})
    far_others = far_tops.at[pl.ds(0, nx - 1)]
    received(far_others, 2)
    q_top = jnp.broadcast_to(jnp.max(far_tops[...], axis=0), (8, 128))
    received(planes, 0)

    inv_top = 1.0 / q_top
    weight = math.sqrt(3.0) / 6.0

    def theta_rows(r, carry):
        rows = pl.ds(pl.multiple_of(r * 8, 8), 8)
        for lane in range(NZ // 128):
            lanes = pl.ds(lane * 128, 128)
            value = planes[0, rows, lanes] * weight
            position = jnp.maximum(
                (NQ - 1.0) + jnp.log(planes[1, rows, lanes] * inv_top) / STEP, 0.0
            )
            splines = []
            for j in range(-1, NQ + 1):
                offset = jnp.abs(position - float(j))
                wide = jnp.maximum(2.0 - offset, 0.0)
                narrow = jnp.maximum(1.0 - offset, 0.0)
                splines.append(wide * wide * wide - 4.0 * (narrow * narrow * narrow))
            up = [splines[0]]
            for j in range(1, KNOTS - 1):
                up.append(splines[j] + LAM * up[-1])
            down = splines[KNOTS - 1]
            for a in range(NQ - 1, -1, -1):
                below = LAM * down
                thetas[a, rows, lanes] = (up[a + 1] + below) * value
                down = splines[a + 1] + below
        return carry

    lax.fori_loop(0, NY // 8, theta_rows, 0)

    for load in loads[1:]:
        load.wait()
    table_yf = ty_f[...]
    quarter = [pl.ds(pl.multiple_of(g * 128, 128), 128) for g in gys]
    z_part = [pl.ds(pl.multiple_of(g * block_z, 128), block_z) for g in gzs]
    my_line = ix * nz + iz

    for c, (first, count) in spans(FORWARD):
        part = pl.ds(first, count)

        def y_forward(a, carry, first=first):
            mid[a] = left_multiply(table_yf, thetas[first + a])
            return carry

        lax.fori_loop(0, count, y_forward, 0, unroll=True)
        rows = right_multiply(mid[pl.ds(0, count)].reshape(count * NY, NZ), tz, False)
        send1[part] = rows.reshape(count, 2, NY // 2, NZ)

        slot = FIRST_LINES + c
        for dx, dy, dz in ORDER:
            src = send1.at[part, :, gxs[dx] * nz + gzs[dz], quarter[dy]]
            to = {"gx": gxs[dx], "gy": gys[dy], "gz": gzs[dz]}
            send(src, recv1.at[part, :, me, :], slot, to)
        keep(send1.at[part, :, my_line, quarter[0]], recv1.at[part, :, me, :], slot)

    col = lax.broadcasted_iota(jnp.int32, (8, COLS), 1)
    wave_y = jnp.where(col < 128, my_line, my_line + NY // 2)
    wave_z = jnp.where(col < 128, col, col - 128) + iy * 128
    yz2 = wave_squared(wave_y, NY) + wave_squared(wave_z, NZ)
    top_sq = jnp.concatenate([q_top * q_top] * (COLS // 128), axis=1)

    def gain_rows(r, carry):
        rows = pl.ds(pl.multiple_of(r * 8, 8), 8)
        k_sq = wave_squared(lax.broadcasted_iota(jnp.int32, (8, COLS), 0) + r * 8, NX) + yz2
        for s in range(SUMS):
            mass = top_sq * math.exp(-STEP * (2 * NQ - 2 - s))
            value = LOCAL + mass / (k_sq + mass)
            gain[s, rows, :] = value
            for a in range(BACKWARD[0]):
                if 0 <= s - a < NQ:
                    link[a, s - a, rows, :] = coup[a, s - a] * value
        return carry

    lax.fori_loop(0, NX // 8, gain_rows, 0)

    table_xf, table_xi = tx_f[...], tx_i[...]

    def over_y(src, dst, dy, slot):
        if dy:
            send(src, dst, slot, {"gy": gys[dy]})
        else:
            keep(src, dst, slot)

    def over_line(src, part, dx, dz, slot):
        dst = y_in.at[part, :, :, my_line, :]
        if dx or dz:
            send(src, dst, slot, {"gx": gxs[dx], "gz": gzs[dz]})
        else:
            keep(src, dst, slot)

    for c, (first, count) in spans(FORWARD):
        received(recv1.at[pl.ds(first, count)], FIRST_LINES + c)

        def x_forward(a, carry, first=first):
            lines = recv1[first + a]
            lines = jnp.concatenate([lines[0], lines[1]], axis=1)
            spec[first + a] = left_multiply(table_xf, lines)
            return carry

        lax.fori_loop(0, count, x_forward, 0, unroll=True)

    for c, (first, count) in spans(BACKWARD):
        part = pl.ds(first, count)

        def couple(r, carry, first=first, count=count):
            rows = pl.ds(pl.multiple_of(r * 8, 8), 8)
            for lane in range(COLS // 128):
                lanes = pl.ds(lane * 128, 128)
                source = [spec[b, rows, lanes] for b in range(NQ)]
                factor = {}
                for s in range(first, first + count + NQ - 1):
                    if first:
                        factor[s] = gain[s, rows, lanes]
                for a in range(count):
                    total = None
                    for b in range(NQ):
                        if first:
                            weight = coup[first + a, b] * factor[first + a + b]
                        else:
                            weight = link[a, b, rows, lanes]
                        term = weight * source[b]
                        total = term if total is None else total + term
                    prod[a, rows, lanes] = total
            return carry

        lax.fori_loop(0, NX // 8, couple, 0)

        def x_inverse(a, carry, first=first):
            lines = left_multiply(table_xi, prod[a])
            for r in range(2):
                send2[first + a, r] = lines[:, 128 * r : 128 * r + 128].reshape(4, NX // 4, 128)
            return carry

        lax.fori_loop(0, count, x_inverse, 0, unroll=True)

        slot = FIRST_BACK + 3 * c
        if ROUTES[c] == "P":
            for dx, dz in LINE_ORDER:
                src = send2.at[part, :, :, gzs[dz] * nx + gxs[dx], :]
                over_line(src, part, dx, dz, slot)
        else:
            for dy in (2, 1, 3, 0):
                src, dst = send2.at[part, :, gys[dy]], z_in_q.at[part, :, :, quarter[0]]
                over_y(src, dst, dy, slot)

    table_yi = ty_i[...]

    def y_inverse_all(first, count):
        def y_inverse(a, carry):
            planes_of = [
                jnp.concatenate([y_in[first + a, 0, k], y_in[first + a, 1, k]], axis=0)
                for k in range(4)
            ]
            rows = left_multiply(table_yi, jnp.concatenate(planes_of, axis=1))
            for k in range(4):
                y_out[first + a, k] = rows[:, 128 * k : 128 * k + 128]
            return carry

        lax.fori_loop(0, count, y_inverse, 0, unroll=True)

    def rows_for(dy):
        return pl.ds(pl.multiple_of(gys[dy] * block_y, 8), block_y)

    def middle(c, first, count):
        part = pl.ds(first, count)
        slot = FIRST_BACK + 3 * c
        received((y_in if ROUTES[c] == "P" else z_in_q).at[part], slot)
        if ROUTES[c] == "P":
            y_inverse_all(first, count)
            for dy in (2, 1, 3, 0):
                src, dst = y_out.at[part, :, rows_for(dy), :], z_in_p.at[part, :, :, quarter[0]]
                over_y(src, dst, dy, slot + 1)
        else:
            rows = right_multiply(z_in_q[part].reshape(count * NY, NZ), tz, True)
            z_out_q[part] = rows.reshape(count, 2, 4, nx, NZ)
            for dx, dz in LINE_ORDER:
                z_of = z_part[dz]
                src = z_out_q.at[part, :, :, gxs[dx], z_of]
                over_line(src, part, dx, dz, slot + 1)

    def last(c, first, count):
        part = pl.ds(first, count)
        slot = FIRST_BACK + 3 * c
        received((z_in_p if ROUTES[c] == "P" else y_in).at[part], slot + 1)
        if ROUTES[c] == "P":
            rows = right_multiply(z_in_p[part].reshape(count * NY, NZ), tz, True)
            z_out_p[part] = rows.reshape(count, 4, block_y, NZ)
            for dz in (2, 3, 1, 0):
                src, dst = z_out_p.at[part, :, :, z_part[dz]], out.at[part, :, iz]
                if dz:
                    send(src, dst, slot + 2, {"gz": gzs[dz]})
                else:
                    keep(src, dst, slot + 2)
        else:
            y_inverse_all(first, count)
            for dy in (2, 1, 3, 0):
                over_y(y_out.at[part, :, rows_for(dy), :], out.at[part, iy], dy, slot + 2)

    chunks = spans(BACKWARD)
    for k in range(len(chunks) + LAG):
        if k < len(chunks):
            c, (first, count) = chunks[k]
            middle(c, first, count)
        if k >= LAG:
            c, (first, count) = chunks[k - LAG]
            last(c, first, count)

    for c, (first, count) in spans(BACKWARD):
        received(out.at[pl.ds(first, count)], FIRST_BACK + 3 * c + 2)

    sent(2 * (group - 1) * block_y * block_z // COLS, 0)
    pltpu.make_async_copy(others, others, ssem.at[1]).wait()
    pltpu.make_async_copy(far_others, far_others, ssem.at[2]).wait()
    for c, (_, count) in spans(FORWARD):
        sent((devices - 1) * count, FIRST_LINES + c)
    for c, (_, count) in spans(BACKWARD):
        few, many = 3 * 32 * count, (nx * nz - 1) * 4 * count
        for k, rows in enumerate((many, few, few) if ROUTES[c] == "P" else (few, many, few)):
            sent(rows, FIRST_BACK + 3 * c + k)


def write_out(fields, out, sem):
    copies = [pltpu.make_async_copy(fields.at[a], out.at[a], sem.at[a]) for a in range(NQ)]
    for copy in copies:
        copy.start()
    for copy in copies:
        copy.wait()


def solution(mesh):
    sizes = tuple(mesh.shape[axis] for axis in ("gx", "gy", "gz"))
    bz = basis(NZ)
    tz = np.stack(halves(bz))
    by, bx = basis(NY), basis(NX)
    x_rows = np.arange(NX).reshape(8, 4, 4).transpose(1, 2, 0).reshape(-1)
    tables = (tz, left_table(by.T), left_table(by), left_table(bx.T), left_table(bx[x_rows]))

    def body(density, coupling):
        vmem, hbm = (pl.BlockSpec(memory_space=space) for space in (pltpu.VMEM, pltpu.HBM))
        block = density.shape
        fields = pl.pallas_call(
            functools.partial(kernel, sizes),
            out_shape=jax.ShapeDtypeStruct((NQ, 4, block[0] // 4) + block[1:], F32),
            in_specs=[hbm] * (2 + len(tables)),
            out_specs=vmem,
            scratch_shapes=[
                pltpu.VMEM((block[0] + 4, block[1] + 16, block[2]), F32),
                pltpu.VMEM((block[2] + 16, block[0] * block[1]), F32),
                pltpu.VMEM((2, 2, block[0] * block[1]), F32),
                pltpu.VMEM((2, 2, block[0] * block[1]), F32),
                pltpu.VMEM((2, NY, NZ), F32),
                pltpu.VMEM(block, F32),
                pltpu.VMEM((2, 1, 128), F32),
                pltpu.VMEM((sizes[1] * sizes[2], 1, 128), F32),
                pltpu.VMEM((sizes[0], 1, 128), F32),
                pltpu.VMEM((NQ, NY, NZ), F32),
                pltpu.VMEM((max(FORWARD), NY, NZ), F32),
                pltpu.VMEM((NQ, 2, NY // 2, NZ), F32),
                pltpu.VMEM((NQ, 2, NX, 128), F32),
                pltpu.VMEM((NQ, NX, COLS), F32),
                pltpu.VMEM((SUMS, NX, COLS), F32),
                pltpu.VMEM((BACKWARD[0], NQ, NX, COLS), F32),
                pltpu.VMEM((max(BACKWARD), NX, COLS), F32),
                pltpu.VMEM((NQ, 2, 4, NX // 4, 128), F32),
                pltpu.VMEM((NQ, 2, 4, NY // 2, 128), F32),
                pltpu.VMEM((NQ, 4, NY, 128), F32),
                pltpu.VMEM((NQ, 4, NY // 4, NZ), F32),
                pltpu.VMEM((NQ, 2, NX // 4, NZ), F32),
                pltpu.VMEM((NQ, 4, NY // 4, NZ), F32),
                pltpu.VMEM((NQ, 2, 4, NX // 16, NZ), F32),
                pltpu.VMEM(block, F32),
                pltpu.SMEM((NQ, NQ), F32),
                *[pltpu.VMEM(table.shape, BF16) for table in tables],
                pltpu.SemaphoreType.DMA((2 + len(tables),)),
                pltpu.SemaphoreType.DMA((SLOTS,)),
                pltpu.SemaphoreType.DMA((SLOTS,)),
                pltpu.SemaphoreType.DMA((8,)),
                pltpu.SemaphoreType.DMA((8,)),
            ],
            compiler_params=pltpu.CompilerParams(
                collective_id=0, has_side_effects=True, vmem_limit_bytes=40 * 1024 * 1024
            ),
            name="convolve",
        )(*[pltpu.with_memory_space_constraint(x, pltpu.HBM) for x in (density, coupling, *map(jnp.asarray, tables))])
        return pl.pallas_call(
            write_out,
            out_shape=jax.ShapeDtypeStruct((NQ,) + block, F32),
            in_specs=[vmem],
            out_specs=hbm,
            scratch_shapes=[pltpu.SemaphoreType.DMA((NQ,))],
            compiler_params=pltpu.CompilerParams(vmem_limit_bytes=4 * 1024 * 1024),
            cost_estimate=pl.CostEstimate(flops=0, bytes_accessed=8 * NQ * density.size, transcendentals=0),
            name="write_out",
        )(fields.reshape((NQ,) + block))

    placed = (P("gx", "gy", "gz"), P())
    return jax.shard_map(
        body, mesh=mesh, in_specs=placed, out_specs=P(None, "gx", "gy", "gz"), check_vma=False
    )
```
